32 devices in a mesh: rep: 4 (over y, x), expert: 8 (over z, core).
Axes of the slice: x: 2, y: 2, z: 4, core: 2. Of those that a mesh axis runs over, the one named last changes fastest.
Arguments:
- tokens: bfloat16 [4096, 1536], P(('rep', 'expert')), may hold values from -6 to 6
- routes: int32 [4096, 4], P(('rep', 'expert')), may hold values from 0 to 7, all different within a row; in each aligned block of 128 rows (0 to 127, 128 to 255, ...) at most 80 rows name the same one
- gates: bfloat16 [4096, 4], P(('rep', 'expert')), may hold values from 0.049804688 to 1
- output_grad: bfloat16 [4096, 1536], P(('rep', 'expert')), may hold values from -6 to 6
- w_in: bfloat16 [8, 1536, 768], P('expert', 'rep'), may hold values from -0.15625 to 0.15625
- w_out: bfloat16 [8, 384, 1536], P('expert', None, 'rep'), may hold values from -0.3125 to 0.3125
- momentum_in: bfloat16 [8, 1536, 768], P('expert', 'rep'), may hold values from -24 to 24
- momentum_out: bfloat16 [8, 384, 1536], P('expert', None, 'rep'), may hold values from -24 to 24
Outputs:
- token_grad: bfloat16 [4096, 1536], P(('rep', 'expert'))
- gate_grad: bfloat16 [4096, 4], P(('rep', 'expert'))
- new_momentum_in: bfloat16 [8, 1536, 768], P('expert', 'rep')
- new_momentum_out: bfloat16 [8, 384, 1536], P('expert', None, 'rep')
The draws below stay inside these ranges and needn't reach their ends.
Inputs may be any that keep to these rules, and one draw needn't show every extreme that they name: `routes`: each row names 4 different experts. Within the 128 rows of one device no expert is named by more than 80 rows, and on some devices one expert is named by exactly 80 rows.
All inputs are finite; a program needn't handle non-finite values.
Results may differ from the reference program's by a relative error of at most 0.012.
Values may be sent and summed in bfloat16 or wider, within the bound.
No kernel may reach another device: no remote copies, remote signals or barrier semaphores. Data moves between devices by JAX's collectives and lax.ppermute only.
A program may use at most 64 MiB of HBM per device.

```python
import math
import jax
import jax.numpy as jnp
import numpy as np
from jax import lax

D = 1536
FFN = 384
TOP = 4
TOK_DEV = 128
EXPERTS = 8
CAP = 80
TOKENS = 4096
N_REP = 4
N_EXPERT = 8


def block_levels(stream_key, extent, cuts, least, high):
    def one(position, parts):
        heights = jax.random.uniform(jax.random.fold_in(jax.random.fold_in(stream_key, 6), position), (parts,), jnp.float32, least / len(cuts), high / len(cuts))
        return jnp.repeat(jnp.exp(heights), extent[position] // parts).reshape((-1,) + (1,) * (len(extent) - position - 1))

    level = one(*cuts[0])
    for cut in cuts[1:]:
        level = level * one(*cut)
    return level


def deal_out(own_key, own, number, rows, count, top, reach, lean):
    order = jax.random.permutation(own_key, count)
    crowded, usual = portions_of(count, rows * top, reach, lean, True), portions_of(count, rows * top, reach, lean, False)
    places = jnp.arange(count)

    def named(lengths, turn):
        used = int((lengths > 0).sum())
        fixed = max(1, used // 4)
        passed = fixed + (places - fixed + turn * (used - fixed)) % max(1, count - fixed)
        return jnp.zeros((count,), jnp.int32).at[order[jnp.where(places < fixed, places, passed)]].set(jnp.asarray(lengths, jnp.int32))

    lengths = jnp.where(number % 4 == 0, named(crowded, number // 4), named(usual, number - number // 4 - 1))
    mixed = jax.random.permutation(jax.random.fold_in(own, 3), count)
    giver, taker = mixed[0:count // 2 * 2:2], mixed[1:count // 2 * 2:2]
    room = jnp.minimum(lengths[giver] - 1, reach - lengths[taker]) // 2
    room = jnp.where((giver == order[0]) | (taker == order[0]) | (lengths[taker] == 0), 0, jnp.maximum(room, 0))
    passed = jax.random.randint(jax.random.fold_in(own, 4), (count // 2,), 0, 1 << 20) % (room + 1)
    lengths = lengths.at[giver].add(-passed).at[taker].add(passed)
    items = jnp.searchsorted(jnp.cumsum(lengths), jnp.arange(rows * top), side="right").astype(jnp.int32)
    listing = items.reshape(top, rows).T
    listing = listing[jax.random.permutation(jax.random.fold_in(own, 1), rows)]
    turn = jax.random.randint(jax.random.fold_in(own, 2), (rows, 1), 0, top)
    return jnp.take_along_axis(listing, (jnp.arange(top)[None, :] + turn) % top, axis=1)


def portions_of(amount, total, reach, slope, full):
    portions = [(1 << 20) // math.isqrt(standing ** slope) + 1 for standing in range(1, amount + 1)]
    largest = reach if full else min(reach, max(-(-total // amount), total * portions[0] // sum(portions)))
    least = 1 if total - largest >= amount - 1 else 0
    counts, rest = [largest] + [least] * (amount - 1), total - largest - least * (amount - 1)
    while rest > 0:
        movable = [i for i in range(1, amount) if counts[i] < largest] or [i for i in range(1, amount) if counts[i] < reach]
        mass, left = sum([portions[i] for i in movable]), rest
        for i in movable:
            more = min(reach - counts[i], max(1, left * portions[i] // mass), rest)
            counts[i] = counts[i] + more
            rest = rest - more
    return np.array(counts)


def centred(key, shape, spread, reach, cuts=(), held_as=jnp.bfloat16):
    entries = jax.random.normal(key, shape, jnp.float32) * spread
    if len(cuts) > 0:
        entries = block_levels(key, shape, cuts, -0.22, 0.18) * entries
    return jnp.clip(entries, min=-reach, max=reach).astype(held_as)


def setup_inputs(seed: int = 0) -> dict:
    key_of = jax.random.split(jax.random.key(seed), 9)
    tokens = centred(key_of[0], (TOKENS, D), 1.0, 6.0, ((0, 32),))
    routes_keys = jax.random.split(jax.random.fold_in(key_of[1], 1), TOKENS // TOK_DEV)
    routes_turns = jax.random.permutation(jax.random.fold_in(key_of[1], 3), TOKENS // TOK_DEV)
    routes = jax.vmap(lambda own, number: deal_out(jax.random.fold_in(key_of[1], 2), own, number, TOK_DEV, EXPERTS, TOP, CAP, 2))(routes_keys, routes_turns).reshape((TOKENS, TOP))
    gates = jnp.clip(jnp.exp(math.log(1.0) - 2.9996462 * jax.random.uniform(key_of[2], (TOKENS, TOP), jnp.float32) ** block_levels(key_of[2], (TOKENS, TOP), ((0, 32),), -0.2, 0.2)), 0.049804688, 1.0).astype(jnp.bfloat16)
    output_grad = centred(key_of[3], (TOKENS, D), 1.0, 6.0, ((0, 32),))
    w_in = centred(key_of[4], (EXPERTS, D, 2 * FFN), D ** -0.5, 0.15625, ((0, 8), (1, 4)))
    w_out = centred(key_of[5], (EXPERTS, FFN, D), FFN ** -0.5, 0.3125, ((0, 8), (2, 4)))
    momentum_in = centred(key_of[6], (EXPERTS, D, 2 * FFN), 4.0, 24.0, ((0, 8), (1, 4)))
    momentum_out = centred(key_of[7], (EXPERTS, FFN, D), 4.0, 24.0, ((0, 8), (2, 4)))
    return {"tokens": tokens, "routes": routes, "gates": gates, "output_grad": output_grad, "w_in": w_in, "w_out": w_out, "momentum_in": momentum_in, "momentum_out": momentum_out}


def slot_positions(routes):
    flat_routes = routes.reshape(-1)
    one_hot = (flat_routes[:, None] == jnp.arange(EXPERTS, dtype=jnp.int32)[None, :]).astype(jnp.int32)
    earlier = jnp.cumsum(one_hot, axis=0) - one_hot
    return jnp.sum(earlier * one_hot, axis=1).reshape(routes.shape).astype(jnp.int32)


def expert_pass(x_rows, grad_rows, gate_rows, weight_in, weight_out):
    width_ffn = weight_out.shape[0]
    both = jnp.dot(x_rows, weight_in, preferred_element_type=jnp.float32)
    gate_pre = both[:, :width_ffn]
    up_part = both[:, width_ffn:]
    silu_gate = jax.nn.silu(gate_pre)
    hidden = (silu_gate * up_part).astype(jnp.bfloat16)
    expert_out = jnp.dot(hidden, weight_out, preferred_element_type=jnp.float32)
    gate_grad = jnp.sum(expert_out * grad_rows.astype(jnp.float32), axis=1).astype(jnp.bfloat16)
    scaled = (gate_rows.astype(jnp.float32)[:, None] * grad_rows.astype(jnp.float32)).astype(jnp.bfloat16)
    hidden_grad = jnp.dot(scaled, weight_out.T, preferred_element_type=jnp.float32)
    sigma = jax.nn.sigmoid(gate_pre)
    dgu = jnp.concatenate([hidden_grad * up_part * sigma * (1.0 + gate_pre * (1.0 - sigma)), hidden_grad * silu_gate], axis=1).astype(jnp.bfloat16)
    row_grad = jnp.dot(dgu, weight_in.T, preferred_element_type=jnp.float32).astype(jnp.bfloat16)
    part_in = jnp.dot(x_rows.T, dgu, preferred_element_type=jnp.float32).astype(jnp.bfloat16)
    part_out = jnp.dot(hidden.T, scaled, preferred_element_type=jnp.float32).astype(jnp.bfloat16)
    return row_grad, gate_grad, part_in, part_out


def reference(tokens, routes, gates, output_grad, w_in, w_out, momentum_in, momentum_out):
    blocks = N_EXPERT
    per_group = blocks * TOK_DEV
    width = tokens.shape[1]
    sums_in = jnp.zeros(w_in.shape, jnp.float32)
    sums_out = jnp.zeros(w_out.shape, jnp.float32)
    grad_parts = []
    gate_parts = []
    for group in range(N_REP):
        first = group * per_group
        x_group = tokens[first:first + per_group]
        route_group = routes[first:first + per_group]
        gate_group = gates[first:first + per_group]
        dy_group = output_grad[first:first + per_group]
        slots = jax.vmap(slot_positions)(route_group.reshape(blocks, TOK_DEV, TOP)).reshape(per_group, TOP)
        owner = jnp.broadcast_to((jnp.arange(per_group, dtype=jnp.int32) // TOK_DEV)[:, None], (per_group, TOP)).astype(jnp.int32)
        token_ids = jnp.broadcast_to(jnp.arange(per_group, dtype=jnp.int32)[:, None], (per_group, TOP)).astype(jnp.int32)
        choice_ids = jnp.broadcast_to(jnp.arange(TOP, dtype=jnp.int32)[None, :], (per_group, TOP)).astype(jnp.int32)
        table = jnp.full((EXPERTS, blocks, CAP), per_group, jnp.int32).at[route_group, owner, slots].set(token_ids)
        choice_table = jnp.zeros((EXPERTS, blocks, CAP), jnp.int32).at[route_group, owner, slots].set(choice_ids)
        gate_table = jnp.zeros((EXPERTS, blocks, CAP), jnp.bfloat16).at[route_group, owner, slots].set(gate_group)
        zero_row = jnp.zeros((1, width), jnp.bfloat16)
        x_padded = jnp.concatenate([x_group, zero_row], axis=0)
        dy_padded = jnp.concatenate([dy_group, zero_row], axis=0)

        def one_expert(inputs):
            expert_table, expert_gates, weight_in, weight_out = inputs
            picked = expert_table.reshape(-1)
            return expert_pass(x_padded[picked], dy_padded[picked], expert_gates.reshape(-1), weight_in, weight_out)

        row_grads, gate_grads, parts_in, parts_out = lax.map(one_expert, (table, gate_table, w_in, w_out))
        sums_in = sums_in + parts_in.astype(jnp.float32)
        sums_out = sums_out + parts_out.astype(jnp.float32)
        flat_tokens = table.reshape(-1)
        flat_choices = choice_table.reshape(-1)
        token_sum = jnp.zeros((per_group + 1, width), jnp.float32).at[flat_tokens].add(row_grads.reshape(-1, width).astype(jnp.float32))
        grad_parts.append(token_sum[:per_group].astype(jnp.bfloat16))
        gate_table_out = jnp.zeros((per_group + 1, TOP), jnp.bfloat16).at[flat_tokens, flat_choices].set(gate_grads.reshape(-1))
        gate_parts.append(gate_table_out[:per_group])
    token_grad = jnp.concatenate(grad_parts, axis=0)
    gate_grad = jnp.concatenate(gate_parts, axis=0)
    new_momentum_in = (0.9 * momentum_in.astype(jnp.float32) + sums_in).astype(jnp.bfloat16)
    new_momentum_out = (0.9 * momentum_out.astype(jnp.float32) + sums_out).astype(jnp.bfloat16)
    return token_grad, gate_grad, new_momentum_in, new_momentum_out
```

```python
import functools

import jax
import jax.numpy as jnp
from jax import lax
from jax.experimental import pallas as pl
from jax.experimental.pallas import tpu as pltpu
from jax.sharding import PartitionSpec as P

momentum_decay = 0.9
bf16 = jnp.bfloat16
f32 = jnp.float32


def dot(a, b, dims):
    return lax.dot_general(a, b, ((dims[0], dims[1]), ((), ())), preferred_element_type=f32)


def pack_kernel(x_ref, y_ref, routes_ref, gates_ref, out_ref):
    tok = x_ref.shape[0]
    experts = out_ref.shape[0] - 2 * tok
    out_ref[0:tok, :] = x_ref[...]
    out_ref[tok : 2 * tok, :] = y_ref[...]
    ids = lax.broadcasted_iota(jnp.int32, (experts, tok), 0)
    dense = jnp.zeros((experts, tok), f32)
    for k in range(routes_ref.shape[0]):
        row = routes_ref[k : k + 1, :]
        gate = gates_ref[k : k + 1, :].astype(f32)
        dense = dense + jnp.where(ids == row, gate, 0.0)
    tail = jnp.zeros((experts, out_ref.shape[1] - tok), f32)
    out_ref[2 * tok :, :] = jnp.concatenate([dense, tail], axis=1).astype(bf16)


def expert_kernel(pairs, last, *refs):
    ids_ref, refs = refs[0], refs[1:]
    blocks, refs = refs[: 2 * pairs], refs[2 * pairs :]
    (own_ref, one_ref, two_ref, three_a_ref, three_b_ref), refs = refs[:5], refs[5:]
    if last:
        (prev_in_ref, prev_out_ref), refs = refs[:2], refs[2:]
        keep_ref, give_ref, mine_ref, r1a_ref, r1b_ref, r2a_ref, r2b_ref, r3a_ref, r3b_ref = refs[:9]
        refs = refs[9:]
    else:
        keep_ref, give_ref, acc_in_ref, acc_out_ref = refs[:4]
        refs = refs[4:]
    win, wout, xs, ys, dgus, chs = refs[:6]
    if last:
        acc_in_ref, acc_out_ref = refs[6:8]
    rep, expert = ids_ref[0], ids_ref[1]
    shard, ffn = own_ref.shape[0], wout.shape[0]
    half = shard // 2
    width = win.shape[0]
    both_w = win.shape[1]
    experts = keep_ref.shape[1] - (keep_ref.shape[1] // 128) * 128
    tok = keep_ref.shape[1] - experts

    def place(index, ref, lo, rows):
        at = pl.multiple_of(index * shard, 128)
        win[pl.ds(at + lo, rows), :] = ref[:, 0:both_w]
        wout[lo : lo + rows, pl.ds(at, shard)] = ref[:, both_w:]

    place(rep, own_ref, 0, shard)
    place(rep ^ 1, one_ref, 0, shard)
    place(rep ^ 2, two_ref, 0, shard)
    place(rep ^ 3, three_a_ref, 0, half)
    place(rep ^ 3, three_b_ref, half, half)
    columns = []
    for n, block in enumerate(blocks):
        xs[n * tok : (n + 1) * tok, :] = block[0:tok, :]
        ys[n * tok : (n + 1) * tok, :] = block[tok : 2 * tok, :]
        table = block[2 * tok :, 0:tok].astype(f32)
        pick = lax.broadcasted_iota(jnp.int32, table.shape, 0) == expert
        row = jnp.where(pick, table, 0.0)
        columns.append(jnp.sum(row.T, axis=1, keepdims=True))
    for n in range(len(blocks)):
        rows = slice(n * tok, (n + 1) * tok)
        gate = columns[n]
        both = dot(xs[rows, :], win[...], ((1,), (0,)))
        back = dot(ys[rows, :], wout[...], ((1,), (1,)))
        g = both[:, :ffn]
        u = both[:, ffn:]
        s = 1.0 / (1.0 + jnp.exp(-g))
        silu = g * s
        hidden = (silu * u).astype(bf16).astype(f32)
        gate_grad = jnp.sum(hidden * back, axis=1, keepdims=True)
        chs[rows, :] = (hidden * gate).astype(bf16)
        dh = back * gate
        dgus[rows, :ffn] = (dh * u * s * (1.0 + g * (1.0 - s))).astype(bf16)
        dgus[rows, ffn:] = (dh * silu).astype(bf16)
        out = keep_ref if n % 2 == 0 else give_ref
        out[n // 2, 0:tok, :] = dot(dgus[rows, :], win[...], ((1,), (1,))).astype(bf16)
        spread = jnp.broadcast_to(gate_grad, (tok, experts)).T
        pick = lax.broadcasted_iota(jnp.int32, spread.shape, 0) == expert
        spread = jnp.where(pick, spread, 0.0)
        tail = jnp.zeros((experts, width - tok), f32)
        out[n // 2, tok:, :] = jnp.concatenate([spread, tail], axis=1).astype(bf16)
    if not last:
        acc_in_ref[...] = dot(xs[...], dgus[...], ((0,), (0,)))
        acc_out_ref[...] = dot(chs[...], ys[...], ((0,), (0,)))
        return
    acc_in_ref[...] = prev_in_ref[...] + dot(xs[...], dgus[...], ((0,), (0,)))
    acc_out_ref[...] = prev_out_ref[...] + dot(chs[...], ys[...], ((0,), (0,)))

    def fetch(index, ref, lo, rows):
        at = pl.multiple_of(index * shard, 128)
        ref[:, 0:both_w] = acc_in_ref[pl.ds(at + lo, rows), :].astype(bf16)
        ref[:, both_w:] = acc_out_ref[lo : lo + rows, pl.ds(at, shard)].astype(bf16)

    fetch(rep ^ 3, r3a_ref, 0, half)
    fetch(rep ^ 3, r3b_ref, half, half)
    fetch(rep ^ 1, r1a_ref, 0, half)
    fetch(rep ^ 1, r1b_ref, half, half)
    fetch(rep ^ 2, r2a_ref, 0, half)
    fetch(rep ^ 2, r2b_ref, half, half)
    fetch(rep, mine_ref, 0, shard)


def run_experts(ids, blocks, weights, previous, tok, experts, width, ffn):
    last = previous is not None
    pairs = len(blocks) // 2
    shard = weights[0].shape[0]
    cols = weights[0].shape[1]
    both_w = 2 * ffn
    rows = 2 * pairs * tok
    S = jax.ShapeDtypeStruct
    outs = [S((pairs, tok + experts, width), bf16)] * 2
    scratch = [
        pltpu.VMEM((width, both_w), bf16),
        pltpu.VMEM((ffn, width), bf16),
        pltpu.VMEM((rows, width), bf16),
        pltpu.VMEM((rows, width), bf16),
        pltpu.VMEM((rows, both_w), bf16),
        pltpu.VMEM((rows, ffn), bf16),
    ]
    if last:
        outs += [S((shard, cols), bf16)] + [S((shard // 2, cols), bf16)] * 6
        scratch += [pltpu.VMEM((width, both_w), f32), pltpu.VMEM((ffn, width), f32)]
    else:
        outs += [S((width, both_w), f32), S((ffn, width), f32)]
    operands = [ids, *blocks, *weights] + (list(previous) if last else [])
    flops = 2 * rows * width * ffn * 8
    return pl.pallas_call(
        functools.partial(expert_kernel, pairs, last),
        out_shape=outs,
        in_specs=[pl.BlockSpec(memory_space=pltpu.SMEM)]
        + [pl.BlockSpec(memory_space=pltpu.VMEM)] * (len(operands) - 1),
        out_specs=[pl.BlockSpec(memory_space=pltpu.VMEM)] * len(outs),
        scratch_shapes=scratch,
        compiler_params=pltpu.CompilerParams(vmem_limit_bytes=40 * 1024 * 1024),
        cost_estimate=pl.CostEstimate(flops=flops, bytes_accessed=8 * 1024 * 1024, transcendentals=rows * ffn),
        name="experts_last" if last else "experts_first",
    )(*operands)


def per_device_dense(tokens, routes, gates, output_grad, w_in, w_out, momentum_in, momentum_out):
    tok, width = tokens.shape
    ffn = w_out.shape[1]
    experts = lax.axis_size("expert")
    chips = experts // 2
    rep = lax.axis_index("rep")
    expert = lax.axis_index("expert")
    ids = jnp.stack([rep, expert]).astype(jnp.int32)

    def over_rep(value, bits):
        return lax.ppermute(value, "rep", [(i, i ^ bits) for i in range(4)])

    def over_chips(value, chip_pairs):
        return lax.ppermute(
            value, "expert", [(2 * a + c, 2 * b + c) for a, b in chip_pairs for c in range(2)]
        )

    def partner(value):
        return lax.ppermute(value, "expert", [(i, i ^ 1) for i in range(experts)])

    own_w = jnp.concatenate([w_in[0], w_out[0]], axis=1)
    shard = own_w.shape[0]
    half = shard // 2
    one_w = over_rep(own_w, 1)
    two_w = over_rep(own_w, 2)
    block = pl.pallas_call(
        pack_kernel,
        out_shape=jax.ShapeDtypeStruct((2 * tok + experts, width), bf16),
        name="pack_block",
    )(tokens, output_grad, routes.T, gates.T)
    far = over_chips(block, [(z, z ^ 2) for z in range(chips)])
    near = over_chips(block, [(z, z ^ 1) for z in range(chips)])
    middle = over_chips(block, [(1, 2), (2, 1)])
    block_p = partner(block)
    three_a = over_rep(one_w[:half], 2)
    three_b = over_rep(two_w[half:], 1)
    weights = (own_w, one_w, two_w, three_a, three_b)
    ends = over_chips(far, [(2, 3), (1, 0)])
    near_p = partner(near)
    far_p = partner(far)
    at_end = (expert // 2 == 0) | (expert // 2 == chips - 1)
    cross = jnp.where(at_end, ends, middle)
    cross_p = partner(cross)
    keep, give, acc_in, acc_out = run_experts(
        ids, [block, block_p, near, near_p, far, far_p], weights, None, tok, experts, width, ffn
    )
    got = partner(give)
    both = (keep.astype(f32) + got.astype(f32)).astype(bf16)
    home_near = over_chips(both[1], [(z, z ^ 1) for z in range(chips)])
    home_far = over_chips(both[2], [(z, z ^ 2) for z in range(chips)])
    keep2, give2, mine, r1a, r1b, r2a, r2b, r3a, r3b = run_experts(
        ids, [cross, cross_p], weights, (acc_in, acc_out), tok, experts, width, ffn
    )
    s3a = over_rep(r3a, 2)
    s3b = over_rep(r3b, 1)
    t2a = over_rep(r2a, 2)
    t1b = over_rep(r1b, 1)
    got2 = partner(give2)
    both2 = (keep2.astype(f32) + got2.astype(f32)).astype(bf16)
    home_cross = over_chips(both2[0], [(z, z ^ 3) for z in range(chips)])
    r1a = (r1a.astype(f32) + s3a.astype(f32)).astype(bf16)
    r2b = (r2b.astype(f32) + s3b.astype(f32)).astype(bf16)
    t1a = over_rep(r1a, 1)
    t2b = over_rep(r2b, 2)
    total = (
        both[0].astype(f32)
        + home_near.astype(f32)
        + home_far.astype(f32)
        + home_cross.astype(f32)
    )
    token_grad = total[:tok].astype(bf16)
    table = total[tok:, :tok]
    picked = routes.T[:, None, :] == jnp.arange(experts, dtype=jnp.int32)[None, :, None]
    gate_grad = jnp.sum(jnp.where(picked, table[None], 0.0), axis=1).astype(bf16).T
    sum_a = mine[:half].astype(f32) + t1a.astype(f32) + t2a.astype(f32)
    sum_b = mine[half:].astype(f32) + t1b.astype(f32) + t2b.astype(f32)
    summed = jnp.concatenate([sum_a, sum_b], axis=0)
    new_in = (momentum_decay * momentum_in.astype(f32) + summed[None, :, : 2 * ffn]).astype(bf16)
    new_out = (momentum_decay * momentum_out.astype(f32) + summed[None, :, 2 * ffn :]).astype(bf16)
    return token_grad, gate_grad, new_in, new_out


def slot_positions(routes, experts):
    flat_routes = routes.reshape(-1)
    one_hot = (flat_routes[:, None] == jnp.arange(experts, dtype=jnp.int32)[None, :]).astype(
        jnp.int32
    )
    earlier = jnp.cumsum(one_hot, axis=0) - one_hot
    return jnp.sum(earlier * one_hot, axis=1)


def forward_pass(x_rows, weight_in, weight_out):
    width_ffn = weight_out.shape[0]
    both = jnp.dot(x_rows, weight_in, preferred_element_type=jnp.float32)
    gate_pre = both[:, :width_ffn]
    up_part = both[:, width_ffn:]
    silu_gate = jax.nn.silu(gate_pre)
    hidden = (silu_gate * up_part).astype(jnp.bfloat16)
    expert_out = jnp.dot(hidden, weight_out, preferred_element_type=jnp.float32)
    return (gate_pre, up_part, silu_gate, hidden, expert_out)


def per_device_sparse(tokens, routes, gates, output_grad, w_in, w_out, momentum_in, momentum_out):
    tok_dev, width = tokens.shape
    top_count = routes.shape[1]
    senders = lax.axis_size("expert")
    local_count = w_in.shape[0]
    experts = senders * local_count
    capacity = max(2, min(tok_dev, 5 * tok_dev * top_count // (4 * experts)))
    slot_count = experts * capacity
    target = routes.reshape(-1) * capacity + slot_positions(routes, experts)
    token_ids = jnp.repeat(jnp.arange(tok_dev, dtype=jnp.int32), top_count)
    source_row = jnp.full((slot_count,), tok_dev, jnp.int32).at[target].set(token_ids)
    slot_gate = jnp.zeros((slot_count,), jnp.bfloat16).at[target].set(gates.reshape(-1))
    zero_row = jnp.zeros((1, width), jnp.bfloat16)
    sent_tokens = jnp.concatenate([tokens, zero_row], axis=0)[source_row].reshape(
        experts, capacity, width
    )
    sent_grads = jnp.concatenate([output_grad, zero_row], axis=0)[source_row].reshape(
        experts, capacity, width
    )
    sent_gate = slot_gate.reshape(experts, capacity)
    whole_in, whole_out = (
        lax.all_gather(w_in, "rep", axis=1, tiled=True),
        lax.all_gather(w_out, "rep", axis=2, tiled=True),
    )

    def local_rows(received, expert):
        shaped = received.reshape((senders, local_count) + received.shape[1:])
        return shaped[:, expert].reshape((senders * capacity,) + received.shape[2:])

    got_tokens, got_grads, got_gate = (
        lax.all_to_all(sent_tokens, "expert", split_axis=0, concat_axis=0, tiled=True),
        lax.all_to_all(sent_grads, "expert", split_axis=0, concat_axis=0, tiled=True),
        lax.all_to_all(sent_gate, "expert", split_axis=0, concat_axis=0, tiled=True),
    )
    forward = [forward_pass(local_rows(got_tokens, 0), whole_in[0], whole_out[0])]
    expert = 0
    gate_pre, up_part, silu_gate, hidden, expert_out = forward[expert]
    dy_rows = local_rows(got_grads, expert)
    gate_grad = jnp.sum(expert_out * dy_rows.astype(jnp.float32), axis=1).astype(jnp.bfloat16)
    scaled = (
        local_rows(got_gate, expert).astype(jnp.float32)[:, None] * dy_rows.astype(jnp.float32)
    ).astype(jnp.bfloat16)
    scaled_rows = [scaled]
    gate_rows = [gate_grad]
    parts_out = [
        lax.dot_general(
            hidden, scaled, (((0,), (0,)), ((), ())), preferred_element_type=jnp.float32
        )
    ]
    grad_out_all = jnp.stack(parts_out)
    summed_out = lax.psum_scatter(
        grad_out_all.astype(jnp.bfloat16), "rep", scatter_dimension=2, tiled=True
    ).astype(jnp.float32)
    expert = 0
    gate_pre, up_part, silu_gate, hidden, expert_out = forward[expert]
    hidden_grad = lax.dot_general(
        scaled_rows[expert],
        whole_out[expert],
        (((1,), (1,)), ((), ())),
        preferred_element_type=jnp.float32,
    )
    sigma = jax.nn.sigmoid(gate_pre)
    dgu = jnp.concatenate(
        [hidden_grad * up_part * sigma * (1.0 + gate_pre * (1.0 - sigma)), hidden_grad * silu_gate],
        axis=1,
    ).astype(jnp.bfloat16)
    row_grad = lax.dot_general(
        dgu, whole_in[expert], (((1,), (1,)), ((), ())), preferred_element_type=jnp.float32
    ).astype(jnp.bfloat16)
    row_grads = row_grad.reshape(senders, 1, capacity, width)
    parts_in = [
        lax.dot_general(
            local_rows(got_tokens, expert),
            dgu,
            (((0,), (0,)), ((), ())),
            preferred_element_type=jnp.float32,
        )
    ]
    grad_in_all = jnp.stack(parts_in)
    back_send = row_grads.reshape(experts, capacity, width)
    gate_send = jnp.stack([item.reshape(senders, capacity) for item in gate_rows], axis=1).reshape(
        experts, capacity
    )
    back_rows, back_gate = (
        lax.all_to_all(back_send, "expert", split_axis=0, concat_axis=0, tiled=True),
        lax.all_to_all(gate_send, "expert", split_axis=0, concat_axis=0, tiled=True),
    )
    picked = back_rows.reshape(slot_count, width)[target].reshape(tok_dev, top_count, width)
    token_grad = jnp.sum(picked.astype(jnp.float32), axis=1).astype(jnp.bfloat16)
    gate_grad_out = back_gate.reshape(-1)[target].reshape(tok_dev, top_count)
    summed_in = lax.psum_scatter(
        grad_in_all.astype(jnp.bfloat16), "rep", scatter_dimension=1, tiled=True
    ).astype(jnp.float32)
    new_momentum_in = (momentum_decay * momentum_in.astype(jnp.float32) + summed_in).astype(
        jnp.bfloat16
    )
    new_momentum_out = (momentum_decay * momentum_out.astype(jnp.float32) + summed_out).astype(
        jnp.bfloat16
    )
    return (token_grad, gate_grad_out, new_momentum_in, new_momentum_out)


def solution(mesh):
    in_specs = (
        P(("rep", "expert"), None),
        P(("rep", "expert"), None),
        P(("rep", "expert"), None),
        P(("rep", "expert"), None),
        P("expert", "rep", None),
        P("expert", None, "rep"),
        P("expert", "rep", None),
        P("expert", None, "rep"),
    )
    out_specs = (
        P(("rep", "expert"), None),
        P(("rep", "expert"), None),
        P("expert", "rep", None),
        P("expert", None, "rep"),
    )
    def per_device(tokens, routes, *rest):
        tok, width = tokens.shape
        experts = mesh.shape["expert"]
        w_in, w_out = rest[2], rest[3]
        dense = (
            experts == 8
            and mesh.shape["rep"] == 4
            and w_in.shape[0] == 1
            and tok == 128
            and width >= tok
            and w_out.shape[1] == w_in.shape[1]
            and w_in.shape[1] % 128 == 0
        )
        step = per_device_dense if dense else per_device_sparse
        return step(tokens, routes, *rest)

    return jax.shard_map(
        per_device, mesh=mesh, in_specs=in_specs, out_specs=out_specs, check_vma=False
    )
```

```python
import functools

import jax
import jax.numpy as jnp
from jax import lax
from jax.experimental import pallas as pl
from jax.experimental.pallas import tpu as pltpu
from jax.sharding import PartitionSpec as P


momentum_decay = 0.9
GROUP = 2
bf16 = jnp.bfloat16
f32 = jnp.float32


def dot(a, b, dims):
    return lax.dot_general(a, b, ((dims[0], dims[1]), ((), ())), preferred_element_type=f32)


def pack_kernel(x_ref, y_ref, routes_ref, gates_ref, out_ref):
    tok = x_ref.shape[0]
    experts = out_ref.shape[0] - 2 * tok
    out_ref[0:tok, :] = x_ref[...]
    out_ref[tok : 2 * tok, :] = y_ref[...]
    ids = lax.broadcasted_iota(jnp.int32, (experts, tok), 0)
    dense = jnp.zeros((experts, tok), f32)
    for k in range(routes_ref.shape[0]):
        row = routes_ref[k : k + 1, :]
        gate = gates_ref[k : k + 1, :].astype(f32)
        dense = dense + jnp.where(ids == row, gate, 0.0)
    tail = jnp.zeros((experts, out_ref.shape[1] - tok), f32)
    out_ref[2 * tok :, :] = jnp.concatenate([dense, tail], axis=1).astype(bf16)


def expert_kernel(pairs, last, *refs):
    ids_ref, refs = refs[0], refs[1:]
    n_blocks = 4 if last else 2 * pairs
    blocks, refs = refs[:n_blocks], refs[n_blocks:]
    pieces, refs = refs[:8], refs[8:]
    if last:
        (prev_in_ref, prev_out_ref), refs = refs[:2], refs[2:]
        keep_ref, give_ref, mine_ref, r1a_ref, r1b_ref, r2a_ref, r2b_ref, r3a_ref, r3b_ref = refs[:9]
        refs = refs[9:]
    else:
        keep_ref, give_ref, acc_in_ref, acc_out_ref = refs[:4]
        refs = refs[4:]
    win, wout, xs, ys, dgus, chs = refs[:6]
    if last:
        acc_in_ref, acc_out_ref = refs[6:8]
    rep, expert = ids_ref[0], ids_ref[1]
    half, ffn = pieces[0].shape[0], wout.shape[0]
    shard = 2 * half
    width = win.shape[0]
    both_w = win.shape[1]
    experts = keep_ref.shape[1] - (keep_ref.shape[1] // 128) * 128
    tok = keep_ref.shape[1] - experts

    def place(index, ref, lo, rows):
        at = pl.multiple_of(index * shard, 128)
        win[pl.ds(at + lo, rows), :] = ref[:, 0:both_w]
        wout[lo : lo + rows, pl.ds(at, shard)] = ref[:, both_w:]

    for j in range(4):
        place(rep ^ j, pieces[2 * j], 0, half)
        place(rep ^ j, pieces[2 * j + 1], half, half)
    columns = []

    def load(n, block):
        xs[n * tok : (n + 1) * tok, :] = block[0:tok, :]
        ys[n * tok : (n + 1) * tok, :] = block[tok : 2 * tok, :]

    def column(table):
        pick = lax.broadcasted_iota(jnp.int32, table.shape, 0) == expert
        columns.append(jnp.sum(jnp.where(pick, table.astype(f32), 0.0).T, axis=1, keepdims=True))

    if last:
        at_end = ids_ref[2] == 1

        @pl.when(at_end)
        def _():
            load(0, blocks[0])
            load(1, blocks[1])

        @pl.when(jnp.logical_not(at_end))
        def _():
            load(0, blocks[2])
            load(1, blocks[3])

        for n in range(2):
            end = blocks[n][2 * tok :, 0:tok].astype(f32)
            mid = blocks[n + 2][2 * tok :, 0:tok].astype(f32)
            column(jnp.where(at_end, end, mid))
    else:
        for n, block in enumerate(blocks):
            load(n, block)
            column(block[2 * tok :, 0:tok])
    step = min(GROUP, 2 * pairs)
    for first in range(0, 2 * pairs, step):
        rows = slice(first * tok, (first + step) * tok)
        gate = jnp.concatenate(columns[first : first + step], axis=0)
        both = dot(xs[rows, :], win[...], ((1,), (0,)))
        back = dot(ys[rows, :], wout[...], ((1,), (1,)))
        g = both[:, :ffn]
        u = both[:, ffn:]
        s = 1.0 / (1.0 + jnp.exp(-g))
        silu = g * s
        hidden = (silu * u).astype(bf16).astype(f32)
        gate_grad = jnp.sum(hidden * back, axis=1, keepdims=True)
        chs[rows, :] = (hidden * gate).astype(bf16)
        dh = back * gate
        dgus[rows, :ffn] = (dh * u * s * (1.0 + g * (1.0 - s))).astype(bf16)
        dgus[rows, ffn:] = (dh * silu).astype(bf16)
        row_grad = dot(dgus[rows, :], win[...], ((1,), (1,))).astype(bf16)
        for n in range(first, first + step):
            part = slice((n - first) * tok, (n - first + 1) * tok)
            out = keep_ref if n % 2 == 0 else give_ref
            out[n // 2, 0:tok, :] = row_grad[part]
            spread = jnp.broadcast_to(gate_grad[part], (tok, experts)).T
            pick = lax.broadcasted_iota(jnp.int32, spread.shape, 0) == expert
            spread = jnp.where(pick, spread, 0.0)
            tail = jnp.zeros((experts, width - tok), f32)
            out[n // 2, tok:, :] = jnp.concatenate([spread, tail], axis=1).astype(bf16)
    if not last:
        acc_in_ref[...] = dot(xs[...], dgus[...], ((0,), (0,)))
        acc_out_ref[...] = dot(chs[...], ys[...], ((0,), (0,)))
        return
    acc_in_ref[...] = prev_in_ref[...] + dot(xs[...], dgus[...], ((0,), (0,)))
    acc_out_ref[...] = prev_out_ref[...] + dot(chs[...], ys[...], ((0,), (0,)))

    def fetch(index, ref, lo, rows):
        at = pl.multiple_of(index * shard, 128)
        ref[:, 0:both_w] = acc_in_ref[pl.ds(at + lo, rows), :].astype(bf16)
        ref[:, both_w:] = acc_out_ref[lo : lo + rows, pl.ds(at, shard)].astype(bf16)

    fetch(rep ^ 3, r3a_ref, 0, half)
    fetch(rep ^ 3, r3b_ref, half, half)
    fetch(rep ^ 1, r1a_ref, 0, half)
    fetch(rep ^ 1, r1b_ref, half, half)
    fetch(rep ^ 2, r2a_ref, 0, half)
    fetch(rep ^ 2, r2b_ref, half, half)
    fetch(rep, mine_ref, 0, shard)


def run_experts(ids, blocks, weights, previous, tok, experts, width, ffn):
    last = previous is not None
    pairs = 1 if last else len(blocks) // 2
    shard = 2 * weights[0].shape[0]
    cols = weights[0].shape[1]
    both_w = 2 * ffn
    rows = 2 * pairs * tok
    S = jax.ShapeDtypeStruct
    outs = [S((pairs, tok + experts, width), bf16)] * 2
    scratch = [
        pltpu.VMEM((width, both_w), bf16),
        pltpu.VMEM((ffn, width), bf16),
        pltpu.VMEM((rows, width), bf16),
        pltpu.VMEM((rows, width), bf16),
        pltpu.VMEM((rows, both_w), bf16),
        pltpu.VMEM((rows, ffn), bf16),
    ]
    if last:
        outs += [S((shard, cols), bf16)] + [S((shard // 2, cols), bf16)] * 6
        scratch += [pltpu.VMEM((width, both_w), f32), pltpu.VMEM((ffn, width), f32)]
    else:
        outs += [S((width, both_w), f32), S((ffn, width), f32)]
    operands = [ids, *blocks, *weights] + (list(previous) if last else [])
    flops = 2 * rows * width * ffn * 8
    return pl.pallas_call(
        functools.partial(expert_kernel, pairs, last),
        out_shape=outs,
        in_specs=[pl.BlockSpec(memory_space=pltpu.SMEM)]
        + [pl.BlockSpec(memory_space=pltpu.VMEM)] * (len(operands) - 1),
        out_specs=[pl.BlockSpec(memory_space=pltpu.VMEM)] * len(outs),
        scratch_shapes=scratch,
        compiler_params=pltpu.CompilerParams(vmem_limit_bytes=(26 if last else 24) * 1024 * 1024),
        cost_estimate=pl.CostEstimate(flops=flops, bytes_accessed=8 * 1024 * 1024, transcendentals=rows * ffn),
        name="experts_last" if last else "experts_first",
    )(*operands)


def finish_kernel(own_ref, t1a_ref, t1b_ref, t2a_ref, t2b_ref, min_ref, mout_ref, nin_ref, nout_ref):
    half = t1a_ref.shape[0]
    cols = min_ref.shape[2]
    for lo, one, two in ((0, t1a_ref, t2a_ref), (half, t1b_ref, t2b_ref)):
        rows = slice(lo, lo + half)
        total = own_ref[rows, :].astype(f32) + one[...].astype(f32) + two[...].astype(f32)
        old_in = momentum_decay * min_ref[0, rows, :].astype(f32)
        old_out = momentum_decay * mout_ref[0, rows, :].astype(f32)
        nin_ref[0, rows, :] = (old_in + total[:, :cols]).astype(bf16)
        nout_ref[0, rows, :] = (old_out + total[:, cols:]).astype(bf16)


def per_device_dense(*args):
    return dense_step(*args)


def dense_step(tokens, routes, gates, output_grad, w_in, w_out, momentum_in, momentum_out):
    tok, width = tokens.shape
    ffn = w_out.shape[1]
    experts = lax.axis_size("expert")
    chips = experts // 2
    rep = lax.axis_index("rep")
    expert = lax.axis_index("expert")
    chip = expert // 2
    at_end = (chip == 0) | (chip == chips - 1)
    ids = jnp.stack([rep, expert, at_end.astype(jnp.int32)]).astype(jnp.int32)

    def over_rep(value, bits):
        return lax.ppermute(value, "rep", [(i, i ^ bits) for i in range(4)])

    def over_chips(value, chip_pairs):
        pairs = [(2 * a + c, 2 * b + c) for a, b in chip_pairs for c in range(2)]
        return lax.ppermute(value, "expert", pairs)

    def partner(value):
        return lax.ppermute(value, "expert", [(i, i ^ 1) for i in range(experts)])

    half = w_in.shape[1] // 2
    own_a = jnp.concatenate([w_in[0, :half], w_out[0, :half]], axis=1)
    own_b = jnp.concatenate([w_in[0, half:], w_out[0, half:]], axis=1)
    w1a = over_rep(own_a, 1)
    w2b = over_rep(own_b, 2)
    block = pl.pallas_call(
        pack_kernel,
        out_shape=jax.ShapeDtypeStruct((2 * tok + experts, width), bf16),
        compiler_params=pltpu.CompilerParams(vmem_limit_bytes=6 * 1024 * 1024),
        name="pack_block",
    )(tokens, output_grad, routes.T, gates.T)
    far = over_chips(block, [(z, z ^ 2) for z in range(chips)])
    w1b = over_rep(own_b, 1)
    w2a = over_rep(own_a, 2)
    near = over_chips(block, [(z, z ^ 1) for z in range(chips)])
    block_p = partner(block)
    middle = over_chips(block, [(1, 2), (2, 1)])
    w3a = over_rep(w1a, 2)
    w3b = over_rep(w2b, 1)
    weights = (own_a, own_b, w1a, w1b, w2a, w2b, w3a, w3b)
    near_p = partner(near)
    ends = over_chips(far, [(2, 3), (1, 0)])
    far_p = partner(far)
    keep, give, acc_in, acc_out = run_experts(
        ids, [block, block_p, near, near_p, far, far_p], weights, None, tok, experts, width, ffn
    )
    got = partner(give)
    both = (keep.astype(f32) + got.astype(f32)).astype(bf16)
    home_near = over_chips(both[1], [(z, z ^ 1) for z in range(chips)])
    home_far = over_chips(both[2], [(z, z ^ 2) for z in range(chips)])
    middle_p = partner(middle)
    ends_p = partner(ends)
    keep2, give2, mine, r1a, r1b, r2a, r2b, r3a, r3b = run_experts(
        ids, [ends, ends_p, middle, middle_p], weights, (acc_in, acc_out), tok, experts, width, ffn
    )
    s3a = over_rep(r3a, 2)
    s3b = over_rep(r3b, 1)
    t2a = over_rep(r2a, 2)
    t1b = over_rep(r1b, 1)
    got2 = partner(give2)
    both2 = (keep2.astype(f32) + got2.astype(f32)).astype(bf16)
    home_cross = over_chips(both2[0], [(z, z ^ 3) for z in range(chips)])
    t1a = over_rep((r1a.astype(f32) + s3a.astype(f32)).astype(bf16), 1)
    t2b = over_rep((r2b.astype(f32) + s3b.astype(f32)).astype(bf16), 2)
    parts = (both[0], home_near, home_far, home_cross)
    token_grad = sum(p[:tok].astype(f32) for p in parts).astype(bf16)
    table = sum(p[tok:, :tok].astype(f32) for p in parts)
    picked = routes.T[:, None, :] == jnp.arange(experts, dtype=jnp.int32)[None, :, None]
    gate_grad = jnp.sum(jnp.where(picked, table[None], 0.0), axis=1).astype(bf16).T
    new_in, new_out = pl.pallas_call(
        finish_kernel,
        out_shape=[
            jax.ShapeDtypeStruct(momentum_in.shape, bf16),
            jax.ShapeDtypeStruct(momentum_out.shape, bf16),
        ],
        compiler_params=pltpu.CompilerParams(vmem_limit_bytes=10 * 1024 * 1024),
        name="finish",
    )(mine, t1a, t1b, t2a, t2b, momentum_in, momentum_out)
    return token_grad, gate_grad, new_in, new_out


def slot_positions(routes, experts):
    flat_routes = routes.reshape(-1)
    one_hot = (flat_routes[:, None] == jnp.arange(experts, dtype=jnp.int32)[None, :]).astype(
        jnp.int32
    )
    earlier = jnp.cumsum(one_hot, axis=0) - one_hot
    return jnp.sum(earlier * one_hot, axis=1)


def forward_pass(x_rows, weight_in, weight_out):
    width_ffn = weight_out.shape[0]
    both = jnp.dot(x_rows, weight_in, preferred_element_type=jnp.float32)
    gate_pre = both[:, :width_ffn]
    up_part = both[:, width_ffn:]
    silu_gate = jax.nn.silu(gate_pre)
    hidden = (silu_gate * up_part).astype(jnp.bfloat16)
    expert_out = jnp.dot(hidden, weight_out, preferred_element_type=jnp.float32)
    return (gate_pre, up_part, silu_gate, hidden, expert_out)


def per_device_sparse(tokens, routes, gates, output_grad, w_in, w_out, momentum_in, momentum_out):
    tok_dev, width = tokens.shape
    top_count = routes.shape[1]
    senders = lax.axis_size("expert")
    local_count = w_in.shape[0]
    experts = senders * local_count
    capacity = max(2, min(tok_dev, 5 * tok_dev * top_count // (4 * experts)))
    slot_count = experts * capacity
    target = routes.reshape(-1) * capacity + slot_positions(routes, experts)
    token_ids = jnp.repeat(jnp.arange(tok_dev, dtype=jnp.int32), top_count)
    source_row = jnp.full((slot_count,), tok_dev, jnp.int32).at[target].set(token_ids)
    slot_gate = jnp.zeros((slot_count,), jnp.bfloat16).at[target].set(gates.reshape(-1))
    zero_row = jnp.zeros((1, width), jnp.bfloat16)
    sent_tokens = jnp.concatenate([tokens, zero_row], axis=0)[source_row].reshape(
        experts, capacity, width
    )
    sent_grads = jnp.concatenate([output_grad, zero_row], axis=0)[source_row].reshape(
        experts, capacity, width
    )
    sent_gate = slot_gate.reshape(experts, capacity)
    whole_in, whole_out = (
        lax.all_gather(w_in, "rep", axis=1, tiled=True),
        lax.all_gather(w_out, "rep", axis=2, tiled=True),
    )

    def local_rows(received, expert):
        shaped = received.reshape((senders, local_count) + received.shape[1:])
        return shaped[:, expert].reshape((senders * capacity,) + received.shape[2:])

    got_tokens, got_grads, got_gate = (
        lax.all_to_all(sent_tokens, "expert", split_axis=0, concat_axis=0, tiled=True),
        lax.all_to_all(sent_grads, "expert", split_axis=0, concat_axis=0, tiled=True),
        lax.all_to_all(sent_gate, "expert", split_axis=0, concat_axis=0, tiled=True),
    )
    forward = [forward_pass(local_rows(got_tokens, 0), whole_in[0], whole_out[0])]
    expert = 0
    gate_pre, up_part, silu_gate, hidden, expert_out = forward[expert]
    dy_rows = local_rows(got_grads, expert)
    gate_grad = jnp.sum(expert_out * dy_rows.astype(jnp.float32), axis=1).astype(jnp.bfloat16)
    scaled = (
        local_rows(got_gate, expert).astype(jnp.float32)[:, None] * dy_rows.astype(jnp.float32)
    ).astype(jnp.bfloat16)
    scaled_rows = [scaled]
    gate_rows = [gate_grad]
    parts_out = [
        lax.dot_general(
            hidden, scaled, (((0,), (0,)), ((), ())), preferred_element_type=jnp.float32
        )
    ]
    grad_out_all = jnp.stack(parts_out)
    summed_out = lax.psum_scatter(
        grad_out_all.astype(jnp.bfloat16), "rep", scatter_dimension=2, tiled=True
    ).astype(jnp.float32)
    expert = 0
    gate_pre, up_part, silu_gate, hidden, expert_out = forward[expert]
    hidden_grad = lax.dot_general(
        scaled_rows[expert],
        whole_out[expert],
        (((1,), (1,)), ((), ())),
        preferred_element_type=jnp.float32,
    )
    sigma = jax.nn.sigmoid(gate_pre)
    dgu = jnp.concatenate(
        [hidden_grad * up_part * sigma * (1.0 + gate_pre * (1.0 - sigma)), hidden_grad * silu_gate],
        axis=1,
    ).astype(jnp.bfloat16)
    row_grad = lax.dot_general(
        dgu, whole_in[expert], (((1,), (1,)), ((), ())), preferred_element_type=jnp.float32
    ).astype(jnp.bfloat16)
    row_grads = row_grad.reshape(senders, 1, capacity, width)
    parts_in = [
        lax.dot_general(
            local_rows(got_tokens, expert),
            dgu,
            (((0,), (0,)), ((), ())),
            preferred_element_type=jnp.float32,
        )
    ]
    grad_in_all = jnp.stack(parts_in)
    back_send = row_grads.reshape(experts, capacity, width)
    gate_send = jnp.stack([item.reshape(senders, capacity) for item in gate_rows], axis=1).reshape(
        experts, capacity
    )
    back_rows, back_gate = (
        lax.all_to_all(back_send, "expert", split_axis=0, concat_axis=0, tiled=True),
        lax.all_to_all(gate_send, "expert", split_axis=0, concat_axis=0, tiled=True),
    )
    picked = back_rows.reshape(slot_count, width)[target].reshape(tok_dev, top_count, width)
    token_grad = jnp.sum(picked.astype(jnp.float32), axis=1).astype(jnp.bfloat16)
    gate_grad_out = back_gate.reshape(-1)[target].reshape(tok_dev, top_count)
    summed_in = lax.psum_scatter(
        grad_in_all.astype(jnp.bfloat16), "rep", scatter_dimension=1, tiled=True
    ).astype(jnp.float32)
    new_momentum_in = (momentum_decay * momentum_in.astype(jnp.float32) + summed_in).astype(
        jnp.bfloat16
    )
    new_momentum_out = (momentum_decay * momentum_out.astype(jnp.float32) + summed_out).astype(
        jnp.bfloat16
    )
    return (token_grad, gate_grad_out, new_momentum_in, new_momentum_out)


def solution(mesh):
    in_specs = (
        P(("rep", "expert"), None),
        P(("rep", "expert"), None),
        P(("rep", "expert"), None),
        P(("rep", "expert"), None),
        P("expert", "rep", None),
        P("expert", None, "rep"),
        P("expert", "rep", None),
        P("expert", None, "rep"),
    )
    out_specs = (
        P(("rep", "expert"), None),
        P(("rep", "expert"), None),
        P("expert", "rep", None),
        P("expert", None, "rep"),
    )

    small = mesh.shape["expert"] == 8 and mesh.shape["rep"] == 4

    def per_device(*args):
        tok, width = args[0].shape
        w_in, w_out = args[4], args[5]
        lanes = (tok, w_in.shape[1], w_out.shape[1], w_out.shape[2], w_in.shape[2])
        fits = small and tok == 128 and width >= tok and all(n % 128 == 0 for n in lanes)
        dense = fits and w_in.shape[0] == 1 and w_in.shape[1] == w_out.shape[2] == w_out.shape[1]
        return (per_device_dense if dense else per_device_sparse)(*args)

    return jax.shard_map(
        per_device, mesh=mesh, in_specs=in_specs, out_specs=out_specs, check_vma=False
    )
```

```python
import functools

import jax
import jax.numpy as jnp
from jax import lax
from jax.experimental import pallas as pl
from jax.experimental.pallas import tpu as pltpu
from jax.sharding import PartitionSpec as P


momentum_decay = 0.9
bf16 = jnp.bfloat16
f32 = jnp.float32
MIB = 1024 * 1024


def dot(a, b, left, right):
    return lax.dot_general(a, b, (((left,), (right,)), ((), ())), preferred_element_type=f32)


def call(kernel, operands, outs, scratch=(), mib=8, scalars=0, flops=0, far=0):
    specs = [pl.BlockSpec(memory_space=pltpu.SMEM)] * scalars
    specs += [pl.BlockSpec(memory_space=pltpu.VMEM)] * (len(operands) - scalars - far)
    specs += [pl.BlockSpec(memory_space=pltpu.HBM)] * far
    return pl.pallas_call(
        kernel,
        out_shape=[jax.ShapeDtypeStruct(shape, dtype) for shape, dtype in outs],
        in_specs=specs,
        out_specs=[pl.BlockSpec(memory_space=pltpu.VMEM)] * len(outs),
        scratch_shapes=[pltpu.VMEM(*item) if isinstance(item, tuple) else item for item in scratch],
        compiler_params=pltpu.CompilerParams(vmem_limit_bytes=mib * MIB),
        cost_estimate=pl.CostEstimate(flops=flops, bytes_accessed=4 * MIB, transcendentals=0),
    )(*operands)


def stage_kernel(routes_hbm, gates_hbm, x_hbm, y_hbm, win_hbm, wout_hbm, *refs):
    x_ref, block_ref, win_ref, wout_ref, routes_ref, gates_ref, sems = refs
    tok = x_ref.shape[0]
    experts = block_ref.shape[0] - tok
    moves = (
        (routes_hbm, routes_ref),
        (gates_hbm, gates_ref),
        (y_hbm, block_ref.at[0:tok]),
        (x_hbm, x_ref),
        (win_hbm, win_ref),
        (wout_hbm, wout_ref),
    )
    copies = [pltpu.make_async_copy(src, dst, sems.at[i]) for i, (src, dst) in enumerate(moves)]
    for copy in copies:
        copy.start()
    copies[0].wait()
    copies[1].wait()
    ids = lax.broadcasted_iota(jnp.int32, (experts, tok), 0)
    dense = jnp.zeros((experts, tok), f32)
    for k in range(routes_ref.shape[0]):
        gate = gates_ref[k : k + 1, :].astype(f32)
        dense = dense + jnp.where(ids == routes_ref[k : k + 1, :], gate, 0.0)
    tail = jnp.zeros((experts, block_ref.shape[1] - tok), f32)
    block_ref[tok:, :] = jnp.concatenate([dense, tail], axis=1).astype(bf16)
    for copy in copies[2:]:
        copy.wait()


def is_end(expert, chips):
    chip = lax.shift_right_logical(expert, 1)
    return (chip == 0) | (chip == chips - 1)


def gate_column(table, expert):
    pick = lax.broadcasted_iota(jnp.int32, table.shape, 0) == expert
    return jnp.sum(jnp.where(pick, table.astype(f32), 0.0).T, axis=1, keepdims=True)


def gate_table(column, experts, expert):
    spread = jnp.broadcast_to(column, (column.shape[0], experts)).T
    pick = lax.broadcasted_iota(jnp.int32, spread.shape, 0) == expert
    return jnp.where(pick, spread, 0.0)


def write_rows(out, row_grad, table):
    tok = row_grad.shape[0]
    out[0:tok, :] = row_grad
    tail = jnp.zeros((table.shape[0], out.shape[1] - tok), f32)
    out[tok:, :] = jnp.concatenate([table, tail], axis=1).astype(bf16)


def activations(both):
    ffn = both.shape[1] // 2
    g, u = both[:, :ffn], both[:, ffn:]
    s = 1.0 / (1.0 + jnp.exp(-g))
    silu = g * s
    hidden = (silu * u).astype(bf16)
    return silu, u * s * (1.0 + g * (1.0 - s)), hidden


def block_step(tables, expert, x, y, win, wout, keep_ref, give_ref, dgu_ref, ch_ref):
    tok, ffn = x.shape[0] // 2, wout.shape[0]
    experts = tables[0].shape[0]
    gate = jnp.concatenate([gate_column(table, expert) for table in tables], axis=0)
    silu, slope, hidden = activations(dot(x, win[...], 1, 0))
    back = dot(y, wout[...], 1, 1)
    gate_grad = jnp.sum(hidden.astype(f32) * back, axis=1, keepdims=True)
    ch_ref[...] = (hidden.astype(f32) * gate).astype(bf16)
    dh = back * gate
    dgu_ref[:, :ffn] = (dh * slope).astype(bf16)
    dgu_ref[:, ffn:] = (dh * silu).astype(bf16)
    row_grad = dot(dgu_ref[...], win[...], 1, 1).astype(bf16)
    for i, out in enumerate((keep_ref, give_ref)):
        part = slice(i * tok, (i + 1) * tok)
        write_rows(out, row_grad[part], gate_table(gate_grad[part], experts, expert))


def own_kernel(ids_ref, x0, x1, y0, y1, *refs):
    in_pieces, out_pieces = refs[0:4], refs[4:8]
    keep_ref, give_ref, dgu_ref, ch_ref, win, wout = refs[8:]
    rep, expert = ids_ref[0], ids_ref[1]
    shard = wout.shape[1] // 4
    for j in range(4):
        at = pl.multiple_of((rep ^ j) * shard, 128)
        win[pl.ds(at, shard), :] = in_pieces[j][0]
        wout[:, pl.ds(at, shard)] = out_pieces[j][0]
    tok = x0.shape[0]
    tables = [ref[tok:, 0:tok] for ref in (y0, y1)]
    x, y = (jnp.concatenate([ref[0:tok, :] for ref in pair], axis=0) for pair in ((x0, x1), (y0, y1)))
    block_step(tables, expert, x, y, win, wout, keep_ref, give_ref, dgu_ref, ch_ref)


def rest_kernel(ids_ref, *refs):
    blocks, (own_dgu, own_ch, win, wout), refs = (refs[0:4], refs[4:8], refs[8:12]), refs[12:16], refs[16:]
    keep_ref, give_ref, acc_in_ref, acc_out_ref, xs, ys, dgus, chs = refs
    tok = blocks[0][0].shape[0]
    rows = 2 * tok
    dgus[0:rows, :] = own_dgu[...]
    chs[0:rows, :] = own_ch[...]
    for n, (x0, x1, y0, y1) in enumerate(blocks):
        at = n * rows
        for i, (xr, yr) in enumerate(((x0, y0), (x1, y1))):
            xs[at + i * tok : at + (i + 1) * tok, :] = xr[...]
            ys[at + i * tok : at + (i + 1) * tok, :] = yr[0:tok, :]
    for n in (1, 2):
        part = slice(n * rows, (n + 1) * rows)
        outs = (keep_ref.at[n - 1], give_ref.at[n - 1], dgus.at[part], chs.at[part])
        x, y = xs[part, :], ys[part, :]
        tables = [ref[tok:, 0:tok] for ref in blocks[n][2:]]
        block_step(tables, ids_ref[1], x, y, win, wout, *outs)
    acc_in_ref[...] = dot(xs[...], dgus[...], 0, 0)
    acc_out_ref[...] = dot(chs[...], ys[...], 0, 0)


def forward_kernel(chips, ids_ref, e0, e1, m0, m1, win, xs, silu_ref, slope_ref, hidden_ref):
    tok = e0.shape[0]
    at_end = is_end(ids_ref[1], chips)

    @pl.when(at_end)
    def _():
        xs[0:tok, :] = e0[...]
        xs[tok:, :] = e1[...]

    @pl.when(jnp.logical_not(at_end))
    def _():
        xs[0:tok, :] = m0[...]
        xs[tok:, :] = m1[...]

    silu_ref[...], slope_ref[...], hidden_ref[...] = activations(dot(xs[...], win[...], 1, 0))


def shard_grads(refs, acc_in_ref, acc_out_ref, xs, ys, dgus, chs, index, half):
    shard = 2 * half
    at = pl.multiple_of(index * shard, 128)
    part_in = acc_in_ref[pl.ds(at, shard), :] + dot(xs[:, pl.ds(at, shard)], dgus[...], 0, 0)
    part_out = acc_out_ref[:, pl.ds(at, shard)] + dot(chs[...], ys[:, pl.ds(at, shard)], 0, 0)
    cols = part_in.shape[1]
    for n, ref in enumerate(refs):
        rows = slice(n * ref.shape[0], (n + 1) * ref.shape[0])
        ref[:, 0:cols] = part_in[rows].astype(bf16)
        ref[:, cols:] = part_out[rows].astype(bf16)


def grad_kernel(chips, ids_ref, e0, e1, m0, m1, xs, silu, slope, hidden, wout, acc_in, acc_out, *refs):
    r3a_ref, r3b_ref, dgus, chs, ys, tab_ref = refs
    tok = ys.shape[0] // 2
    rep, expert = ids_ref[0], ids_ref[1]
    at_end = is_end(ids_ref[1], chips)
    ffn, experts = wout.shape[0], tab_ref.shape[1]

    @pl.when(at_end)
    def _():
        ys[0:tok, :] = e0[0:tok, :]
        ys[tok:, :] = e1[0:tok, :]

    @pl.when(jnp.logical_not(at_end))
    def _():
        ys[0:tok, :] = m0[0:tok, :]
        ys[tok:, :] = m1[0:tok, :]

    columns = []
    for end, mid in ((e0, m0), (e1, m1)):
        table = jnp.where(at_end, end[tok:, 0:tok].astype(f32), mid[tok:, 0:tok].astype(f32))
        columns.append(gate_column(table, expert))
    gate = jnp.concatenate(columns, axis=0)
    back = dot(ys[...], wout[...], 1, 1)
    gate_grad = jnp.sum(hidden[...].astype(f32) * back, axis=1, keepdims=True)
    chs[...] = (hidden[...].astype(f32) * gate).astype(bf16)
    dh = back * gate
    dgus[:, :ffn] = (dh * slope[...]).astype(bf16)
    dgus[:, ffn:] = (dh * silu[...]).astype(bf16)
    for i in range(2):
        tab_ref[i] = gate_table(gate_grad[i * tok : (i + 1) * tok], experts, expert)
    half = r3a_ref.shape[0]
    shard_grads((r3a_ref, r3b_ref), acc_in, acc_out, xs, ys, dgus, chs, rep ^ 3, half)


def other_grads_kernel(ids_ref, xs, ys, dgus, chs, acc_in, acc_out, mine_ref, r1a_ref, r1b_ref, r2a_ref, r2b_ref):
    rep, half = ids_ref[0], r1a_ref.shape[0]
    args = (acc_in, acc_out, xs, ys, dgus, chs)
    shard_grads((r1a_ref, r1b_ref), *args, rep ^ 1, half)
    shard_grads((r2a_ref, r2b_ref), *args, rep ^ 2, half)
    shard_grads((mine_ref,), *args, rep, half)


def rows_kernel(dgus, win, tab_ref, keep_ref, give_ref):
    tok = dgus.shape[0] // 2
    row_grad = dot(dgus[...], win[...], 1, 1).astype(bf16)
    for i, out in enumerate((keep_ref, give_ref)):
        write_rows(out, row_grad[i * tok : (i + 1) * tok], tab_ref[i])


def finish_kernel(own_ref, t1a_ref, t1b_ref, t2a_ref, t2b_ref, min_ref, mout_ref, nin_ref, nout_ref):
    half = t1a_ref.shape[0]
    cols = min_ref.shape[2]
    for lo, one, two in ((0, t1a_ref, t2a_ref), (half, t1b_ref, t2b_ref)):
        rows = slice(lo, lo + half)
        total = own_ref[rows, :].astype(f32) + one[...].astype(f32) + two[...].astype(f32)
        old_in = momentum_decay * min_ref[0, rows, :].astype(f32)
        old_out = momentum_decay * mout_ref[0, rows, :].astype(f32)
        nin_ref[0, rows, :] = (old_in + total[:, :cols]).astype(bf16)
        nout_ref[0, rows, :] = (old_out + total[:, cols:]).astype(bf16)


def per_device_dense(*args):
    return dense_step(*args)


def dense_step(tokens, routes, gates, output_grad, w_in, w_out, momentum_in, momentum_out):
    tok, width = tokens.shape
    ffn, both_w = w_out.shape[1], w_in.shape[2]
    shard = w_in.shape[1]
    half = shard // 2
    cols = both_w + shard
    experts = lax.axis_size("expert")
    chips = experts // 2
    rep = lax.axis_index("rep")
    expert = lax.axis_index("expert")
    ids = jnp.stack([rep, expert]).astype(jnp.int32)

    def over_rep(value, bits):
        return lax.ppermute(value, "rep", [(i, i ^ bits) for i in range(4)])

    def over_chips(value, chip_pairs):
        pairs = [(2 * a + c, 2 * b + c) for a, b in chip_pairs for c in range(2)]
        return lax.ppermute(value, "expert", pairs)

    def partner(value):
        return lax.ppermute(value, "expert", [(i, i ^ 1) for i in range(experts)])

    to_far = [(z, z ^ 2) for z in range(chips)]
    to_near = [(z, z ^ 1) for z in range(chips)]
    to_cross = [(z, z ^ 3) for z in range(chips)]
    to_middle = [(1, 2), (2, 1)]
    to_ends = [(2, 3), (1, 0)]

    far_x = over_chips(tokens, to_far)
    w1in = over_rep(w_in, 1)
    w2in = over_rep(w_in, 2)
    near_x = over_chips(tokens, to_near)
    top = routes.shape[1]
    sources = [routes.T, gates.T, tokens, output_grad, w_in, w_out]
    own_x, own_y, own_in, own_out = call(
        stage_kernel,
        sources,
        [((tok, width), bf16), ((tok + experts, width), bf16), (w_in.shape, bf16), (w_out.shape, bf16)],
        [((top, tok), jnp.int32), ((top, tok), bf16), pltpu.SemaphoreType.DMA((len(sources),))],
        mib=2,
        far=len(sources),
    )
    far_y = over_chips(own_y, to_far)
    near_y = over_chips(own_y, to_near)
    w1out = over_rep(w_out, 1)
    w2out = over_rep(w_out, 2)
    middle_x = over_chips(tokens, to_middle)
    own_xp = partner(own_x)
    own_yp = partner(own_y)
    w3in = over_rep(w1in, 2)
    ends_x = over_chips(far_x, to_ends)
    w3out = over_rep(w2out, 1)
    far_xp = partner(far_x)
    near_xp = partner(near_x)
    middle_y = over_chips(own_y, to_middle)
    ends_y = over_chips(far_y, to_ends)
    far_yp = partner(far_y)
    near_yp = partner(near_y)
    rows = 2 * tok
    block = ((tok + experts, width), bf16)
    flops = 5 * rows * width * both_w
    own_blocks = [own_x, own_xp, own_y, own_yp]
    keep, give_own, own_dgu, own_ch, win, wout = call(
        own_kernel,
        [ids, *own_blocks, own_in, w1in, w2in, w3in, own_out, w1out, w2out, w3out],
        [block, block, ((rows, both_w), bf16), ((rows, ffn), bf16)]
        + [((width, both_w), bf16), ((ffn, width), bf16)],
        mib=10,
        scalars=1,
        flops=flops,
    )
    got = partner(give_own)
    home_own = (keep.astype(f32) + got.astype(f32)).astype(bf16)
    keep, give, acc_in, acc_out = call(
        rest_kernel,
        [ids, *own_blocks, near_x, near_xp, near_y, near_yp, far_x, far_xp, far_y, far_yp]
        + [own_dgu, own_ch, win, wout],
        [((2, tok + experts, width), bf16)] * 2 + [((width, both_w), f32), ((ffn, width), f32)],
        [((3 * rows, n), bf16) for n in (width, width, both_w, ffn)],
        mib=18,
        scalars=1,
        flops=3 * flops,
    )
    middle_xp = partner(middle_x)
    ends_xp = partner(ends_x)
    got = partner(give)
    home_near, home_far = ((keep[i].astype(f32) + got[i].astype(f32)).astype(bf16) for i in range(2))
    xs, silu, slope, hidden = call(
        functools.partial(forward_kernel, chips),
        [ids, ends_x, ends_xp, middle_x, middle_xp, win],
        [((rows, width), bf16), ((rows, ffn), f32), ((rows, ffn), f32), ((rows, ffn), bf16)],
        scalars=1,
        flops=2 * rows * width * both_w,
    )
    middle_yp = partner(middle_y)
    ends_yp = partner(ends_y)
    home_near = over_chips(home_near, to_near)
    home_far = over_chips(home_far, to_far)
    r3a, r3b, dgus, chs, ys, table = call(
        functools.partial(grad_kernel, chips),
        [ids, ends_y, ends_yp, middle_y, middle_yp, xs, silu, slope, hidden, wout]
        + [acc_in, acc_out],
        [((half, cols), bf16)] * 2
        + [((rows, both_w), bf16), ((rows, ffn), bf16), ((rows, width), bf16), ((2, experts, tok), f32)],
        mib=8,
        scalars=1,
        flops=rows * width * both_w * 2,
    )
    s3a = over_rep(r3a, 2)
    s3b = over_rep(r3b, 1)
    mine, r1a, r1b, r2a, r2b = call(
        other_grads_kernel,
        [ids, xs, ys, dgus, chs, acc_in, acc_out],
        [((shard, cols), bf16)] + [((half, cols), bf16)] * 4,
        mib=8,
        scalars=1,
        flops=2 * rows * width * both_w,
    )
    keep2, give2 = call(rows_kernel, [dgus, win, table], [block, block])
    got2 = partner(give2)
    t2a = over_rep(r2a, 2)
    t1b = over_rep(r1b, 1)
    last = (keep2.astype(f32) + got2.astype(f32)).astype(bf16)
    home_cross = over_chips(last, to_cross)
    t1a = over_rep((r1a.astype(f32) + s3a.astype(f32)).astype(bf16), 1)
    t2b = over_rep((r2b.astype(f32) + s3b.astype(f32)).astype(bf16), 2)
    parts = (home_own, home_near, home_far, home_cross)
    token_grad = sum(p[:tok].astype(f32) for p in parts).astype(bf16)
    table = sum(p[tok:, :tok].astype(f32) for p in parts)
    picked = routes.T[:, None, :] == jnp.arange(experts, dtype=jnp.int32)[None, :, None]
    gate_grad = jnp.sum(jnp.where(picked, table[None], 0.0), axis=1).astype(bf16).T
    new_in, new_out = call(
        finish_kernel,
        [mine, t1a, t1b, t2a, t2b, momentum_in, momentum_out],
        [(momentum_in.shape, bf16), (momentum_out.shape, bf16)],
    )
    return token_grad, gate_grad, new_in, new_out


def slot_positions(routes, experts):
    flat_routes = routes.reshape(-1)
    one_hot = (flat_routes[:, None] == jnp.arange(experts, dtype=jnp.int32)[None, :]).astype(
        jnp.int32
    )
    earlier = jnp.cumsum(one_hot, axis=0) - one_hot
    return jnp.sum(earlier * one_hot, axis=1)


def forward_pass(x_rows, weight_in, weight_out):
    width_ffn = weight_out.shape[0]
    both = jnp.dot(x_rows, weight_in, preferred_element_type=jnp.float32)
    gate_pre = both[:, :width_ffn]
    up_part = both[:, width_ffn:]
    silu_gate = jax.nn.silu(gate_pre)
    hidden = (silu_gate * up_part).astype(jnp.bfloat16)
    expert_out = jnp.dot(hidden, weight_out, preferred_element_type=jnp.float32)
    return (gate_pre, up_part, silu_gate, hidden, expert_out)


def per_device_sparse(tokens, routes, gates, output_grad, w_in, w_out, momentum_in, momentum_out):
    tok_dev, width = tokens.shape
    top_count = routes.shape[1]
    senders = lax.axis_size("expert")
    local_count = w_in.shape[0]
    experts = senders * local_count
    capacity = max(2, min(tok_dev, 5 * tok_dev * top_count // (4 * experts)))
    slot_count = experts * capacity
    target = routes.reshape(-1) * capacity + slot_positions(routes, experts)
    token_ids = jnp.repeat(jnp.arange(tok_dev, dtype=jnp.int32), top_count)
    source_row = jnp.full((slot_count,), tok_dev, jnp.int32).at[target].set(token_ids)
    slot_gate = jnp.zeros((slot_count,), jnp.bfloat16).at[target].set(gates.reshape(-1))
    zero_row = jnp.zeros((1, width), jnp.bfloat16)
    sent_tokens = jnp.concatenate([tokens, zero_row], axis=0)[source_row].reshape(
        experts, capacity, width
    )
    sent_grads = jnp.concatenate([output_grad, zero_row], axis=0)[source_row].reshape(
        experts, capacity, width
    )
    sent_gate = slot_gate.reshape(experts, capacity)
    whole_in, whole_out = (
        lax.all_gather(w_in, "rep", axis=1, tiled=True),
        lax.all_gather(w_out, "rep", axis=2, tiled=True),
    )

    def local_rows(received, expert):
        shaped = received.reshape((senders, local_count) + received.shape[1:])
        return shaped[:, expert].reshape((senders * capacity,) + received.shape[2:])

    got_tokens, got_grads, got_gate = (
        lax.all_to_all(sent_tokens, "expert", split_axis=0, concat_axis=0, tiled=True),
        lax.all_to_all(sent_grads, "expert", split_axis=0, concat_axis=0, tiled=True),
        lax.all_to_all(sent_gate, "expert", split_axis=0, concat_axis=0, tiled=True),
    )
    forward = [forward_pass(local_rows(got_tokens, 0), whole_in[0], whole_out[0])]
    expert = 0
    gate_pre, up_part, silu_gate, hidden, expert_out = forward[expert]
    dy_rows = local_rows(got_grads, expert)
    gate_grad = jnp.sum(expert_out * dy_rows.astype(jnp.float32), axis=1).astype(jnp.bfloat16)
    scaled = (
        local_rows(got_gate, expert).astype(jnp.float32)[:, None] * dy_rows.astype(jnp.float32)
    ).astype(jnp.bfloat16)
    scaled_rows = [scaled]
    gate_rows = [gate_grad]
    parts_out = [
        lax.dot_general(
            hidden, scaled, (((0,), (0,)), ((), ())), preferred_element_type=jnp.float32
        )
    ]
    grad_out_all = jnp.stack(parts_out)
    summed_out = lax.psum_scatter(
        grad_out_all.astype(jnp.bfloat16), "rep", scatter_dimension=2, tiled=True
    ).astype(jnp.float32)
    expert = 0
    gate_pre, up_part, silu_gate, hidden, expert_out = forward[expert]
    hidden_grad = lax.dot_general(
        scaled_rows[expert],
        whole_out[expert],
        (((1,), (1,)), ((), ())),
        preferred_element_type=jnp.float32,
    )
    sigma = jax.nn.sigmoid(gate_pre)
    dgu = jnp.concatenate(
        [hidden_grad * up_part * sigma * (1.0 + gate_pre * (1.0 - sigma)), hidden_grad * silu_gate],
        axis=1,
    ).astype(jnp.bfloat16)
    row_grad = lax.dot_general(
        dgu, whole_in[expert], (((1,), (1,)), ((), ())), preferred_element_type=jnp.float32
    ).astype(jnp.bfloat16)
    row_grads = row_grad.reshape(senders, 1, capacity, width)
    parts_in = [
        lax.dot_general(
            local_rows(got_tokens, expert),
            dgu,
            (((0,), (0,)), ((), ())),
            preferred_element_type=jnp.float32,
        )
    ]
    grad_in_all = jnp.stack(parts_in)
    back_send = row_grads.reshape(experts, capacity, width)
    gate_send = jnp.stack([item.reshape(senders, capacity) for item in gate_rows], axis=1).reshape(
        experts, capacity
    )
    back_rows, back_gate = (
        lax.all_to_all(back_send, "expert", split_axis=0, concat_axis=0, tiled=True),
        lax.all_to_all(gate_send, "expert", split_axis=0, concat_axis=0, tiled=True),
    )
    picked = back_rows.reshape(slot_count, width)[target].reshape(tok_dev, top_count, width)
    token_grad = jnp.sum(picked.astype(jnp.float32), axis=1).astype(jnp.bfloat16)
    gate_grad_out = back_gate.reshape(-1)[target].reshape(tok_dev, top_count)
    summed_in = lax.psum_scatter(
        grad_in_all.astype(jnp.bfloat16), "rep", scatter_dimension=1, tiled=True
    ).astype(jnp.float32)
    new_momentum_in = (momentum_decay * momentum_in.astype(jnp.float32) + summed_in).astype(
        jnp.bfloat16
    )
    new_momentum_out = (momentum_decay * momentum_out.astype(jnp.float32) + summed_out).astype(
        jnp.bfloat16
    )
    return (token_grad, gate_grad_out, new_momentum_in, new_momentum_out)


def solution(mesh):
    in_specs = (
        P(("rep", "expert"), None),
        P(("rep", "expert"), None),
        P(("rep", "expert"), None),
        P(("rep", "expert"), None),
        P("expert", "rep", None),
        P("expert", None, "rep"),
        P("expert", "rep", None),
        P("expert", None, "rep"),
    )
    out_specs = (
        P(("rep", "expert"), None),
        P(("rep", "expert"), None),
        P("expert", "rep", None),
        P("expert", None, "rep"),
    )

    small = mesh.shape["expert"] == 8 and mesh.shape["rep"] == 4

    def per_device(*args):
        tok, width = args[0].shape
        w_in, w_out = args[4], args[5]
        lanes = (tok, w_in.shape[1], w_out.shape[1], w_out.shape[2], w_in.shape[2])
        fits = small and tok == 128 and width >= tok and all(n % 128 == 0 for n in lanes)
        dense = fits and w_in.shape[0] == 1 and w_in.shape[1] == w_out.shape[2] == w_out.shape[1]
        return (per_device_dense if dense else per_device_sparse)(*args)

    return jax.shard_map(
        per_device, mesh=mesh, in_specs=in_specs, out_specs=out_specs, check_vma=False
    )
```

```python
import functools

import jax
import jax.numpy as jnp
from jax import lax
from jax.experimental import pallas as pl
from jax.experimental.pallas import tpu as pltpu
from jax.sharding import PartitionSpec as P


momentum_decay = 0.9
bf16 = jnp.bfloat16
f32 = jnp.float32
MIB = 1024 * 1024


def dot(a, b, left, right):
    return lax.dot_general(a, b, (((left,), (right,)), ((), ())), preferred_element_type=f32)


def call(kernel, operands, outs, scratch=(), mib=8, scalars=0, flops=0, far=0):
    specs = [pl.BlockSpec(memory_space=pltpu.SMEM)] * scalars
    specs += [pl.BlockSpec(memory_space=pltpu.VMEM)] * (len(operands) - scalars - far)
    specs += [pl.BlockSpec(memory_space=pltpu.HBM)] * far
    return pl.pallas_call(
        kernel,
        out_shape=[jax.ShapeDtypeStruct(shape, dtype) for shape, dtype in outs],
        in_specs=specs,
        out_specs=[pl.BlockSpec(memory_space=pltpu.VMEM)] * len(outs),
        scratch_shapes=[pltpu.VMEM(*item) if isinstance(item, tuple) else item for item in scratch],
        compiler_params=pltpu.CompilerParams(vmem_limit_bytes=mib * MIB),
        cost_estimate=pl.CostEstimate(flops=flops, bytes_accessed=4 * MIB, transcendentals=0),
    )(*operands)


def stage_kernel(routes_hbm, gates_hbm, x_hbm, y_hbm, win_hbm, wout_hbm, *refs):
    x_ref, block_ref, win_ref, wout_ref, routes_ref, gates_ref, y_ref, sems = refs
    tok, width = y_ref.shape
    moves = (
        (routes_hbm, routes_ref),
        (gates_hbm, gates_ref),
        (y_hbm, y_ref),
        (x_hbm, x_ref),
        (win_hbm, win_ref),
        (wout_hbm, wout_ref),
    )
    copies = [pltpu.make_async_copy(src, dst, sems.at[i]) for i, (src, dst) in enumerate(moves)]
    for copy in copies:
        copy.start()
    copies[0].wait()
    copies[1].wait()
    first = width // 128 * tok
    experts = block_ref.shape[0] - first
    ids = lax.broadcasted_iota(jnp.int32, (experts, tok), 0)
    dense = jnp.zeros((experts, tok), f32)
    for k in range(routes_ref.shape[0]):
        gate = gates_ref[k : k + 1, :].astype(f32)
        dense = dense + jnp.where(ids == routes_ref[k : k + 1, :], gate, 0.0)
    block_ref[first:, :] = dense.astype(bf16)
    copies[2].wait()
    for j in range(width // 128):
        block_ref[j * tok : (j + 1) * tok, :] = y_ref[:, j * 128 : (j + 1) * 128]
    for copy in copies[3:]:
        copy.wait()


def stacked(width, tok, experts):
    return (width // 128 * tok + experts, 128)


def unstack(ref, width):
    tok = 128
    return jnp.concatenate([ref[j * tok : (j + 1) * tok, :] for j in range(width // 128)], axis=1)


def is_end(expert, chips):
    chip = lax.shift_right_logical(expert, 1)
    return (chip == 0) | (chip == chips - 1)


def gate_column(table, expert):
    pick = lax.broadcasted_iota(jnp.int32, table.shape, 0) == expert
    return jnp.sum(jnp.where(pick, table.astype(f32), 0.0).T, axis=1, keepdims=True)


def gate_table(column, experts, expert):
    spread = jnp.broadcast_to(column, (column.shape[0], experts)).T
    pick = lax.broadcasted_iota(jnp.int32, spread.shape, 0) == expert
    return jnp.where(pick, spread, 0.0)


def write_rows(out, row_grad, table):
    tok = row_grad.shape[0]
    out[0:tok, :] = row_grad
    tail = jnp.zeros((table.shape[0], out.shape[1] - tok), f32)
    out[tok:, :] = jnp.concatenate([table, tail], axis=1).astype(bf16)


def activations(both):
    ffn = both.shape[1] // 2
    g, u = both[:, :ffn], both[:, ffn:]
    s = 1.0 / (1.0 + jnp.exp(-g))
    silu = g * s
    hidden = (silu * u).astype(bf16)
    return silu, u * s * (1.0 + g * (1.0 - s)), hidden


def back_step(tables, expert, y, acts, win, wout, keep_ref, give_ref, dgu_ref, ch_ref):
    silu, slope, hidden = acts
    tok, ffn, experts = y.shape[0] // 2, wout.shape[0], tables[0].shape[0]
    gate = jnp.concatenate([gate_column(table, expert) for table in tables], axis=0)
    back = dot(y, wout[...], 1, 1)
    gate_grad = jnp.sum(hidden.astype(f32) * back, axis=1, keepdims=True)
    ch_ref[...] = (hidden.astype(f32) * gate).astype(bf16)
    dh = back * gate
    dgu_ref[:, :ffn] = (dh * slope).astype(bf16)
    dgu_ref[:, ffn:] = (dh * silu).astype(bf16)
    row_grad = dot(dgu_ref[...], win[...], 1, 1).astype(bf16)
    for i, out in enumerate((keep_ref, give_ref)):
        part = slice(i * tok, (i + 1) * tok)
        write_rows(out, row_grad[part], gate_table(gate_grad[part], experts, expert))


def own_kernel(ids_ref, x0, x1, y0, y1, *refs):
    in_pieces, out_pieces, refs = refs[0:5], refs[5:9], refs[9:]
    keep_ref, give_ref, dgu_ref, ch_ref, win, wout = refs
    rep, expert = ids_ref[0], ids_ref[1]
    shard, (tok, width) = wout.shape[1] // 4, x0.shape
    cut = in_pieces[3].shape[1]
    for j in range(4):
        at = pl.multiple_of((rep ^ j) * shard, 128)
        wout[:, pl.ds(at, shard)] = out_pieces[j][0]
        if j < 3:
            win[pl.ds(at, shard), :] = in_pieces[j][0]
        else:
            win[pl.ds(at, cut), :] = in_pieces[3][0]
            win[pl.ds(at + cut, shard - cut), :] = in_pieces[4][0]
    tables = [ref[width // 128 * tok :, :] for ref in (y0, y1)]
    x = jnp.concatenate([x0[...], x1[...]], axis=0)
    y = jnp.concatenate([unstack(y0, width), unstack(y1, width)], axis=0)
    acts = activations(dot(x, win[...], 1, 0))
    back_step(tables, expert, y, acts, win, wout, keep_ref, give_ref, dgu_ref, ch_ref)


def early_kernel(n0, n1, f0, f1, win, xs, silu_ref, slope_ref, hidden_ref):
    tok = n0.shape[0]
    for n, ref in enumerate((n0, n1, f0, f1)):
        xs[n * tok : (n + 1) * tok, :] = ref[...]
    silu_ref[...], slope_ref[...], hidden_ref[...] = activations(dot(xs[...], win[...], 1, 0))


def rest_kernel(ids_ref, *refs):
    blocks, (silu, slope, hidden, win, wout), refs = refs[0:4], refs[4:9], refs[9:]
    keep_ref, give_ref, ys, dgus, chs = refs
    rows, width = ys.shape[0] // 2, ys.shape[1]
    tok = rows // 2
    for n in range(2):
        part, pair = slice(n * rows, (n + 1) * rows), blocks[2 * n : 2 * n + 2]
        for i, ref in enumerate(pair):
            ys[n * rows + i * tok : n * rows + (i + 1) * tok, :] = unstack(ref, width)
        tables = [ref[width // 128 * tok :, :] for ref in pair]
        acts = (silu[part, :], slope[part, :], hidden[part, :])
        outs = (keep_ref.at[n], give_ref.at[n], dgus.at[part], chs.at[part])
        back_step(tables, ids_ref[1], ys[part, :], acts, win, wout, *outs)


def sum_kernel(x0, x1, y0, y1, own_dgu, own_ch, more_xs, more_ys, more_dgu, more_ch, *refs):
    acc_in_ref, acc_out_ref, xs, ys, dgus, chs = refs
    tok, width = x0.shape
    rows = 2 * tok
    for i, (x, y) in enumerate(((x0, y0), (x1, y1))):
        xs[i * tok : (i + 1) * tok, :] = x[...]
        ys[i * tok : (i + 1) * tok, :] = unstack(y, width)
    for whole, first, more in ((dgus, own_dgu, more_dgu), (chs, own_ch, more_ch)):
        whole[0:rows, :] = first[...]
        whole[rows:, :] = more[...]
    xs[rows:, :] = more_xs[...]
    ys[rows:, :] = more_ys[...]
    acc_in_ref[...] = dot(xs[...], dgus[...], 0, 0)
    acc_out_ref[...] = dot(chs[...], ys[...], 0, 0)


def forward_kernel(chips, ids_ref, e0, e1, m0, m1, win, xs, silu_ref, slope_ref, hidden_ref):
    tok = e0.shape[0]
    at_end = is_end(ids_ref[1], chips)

    @pl.when(at_end)
    def _():
        xs[0:tok, :] = e0[...]
        xs[tok:, :] = e1[...]

    @pl.when(jnp.logical_not(at_end))
    def _():
        xs[0:tok, :] = m0[...]
        xs[tok:, :] = m1[...]

    silu_ref[...], slope_ref[...], hidden_ref[...] = activations(dot(xs[...], win[...], 1, 0))


def shard_grads(refs, acc_in_ref, acc_out_ref, xs, ys, dgus, chs, index, half):
    shard = 2 * half
    at = pl.multiple_of(index * shard, 128)
    part_in = acc_in_ref[pl.ds(at, shard), :] + dot(xs[:, pl.ds(at, shard)], dgus[...], 0, 0)
    part_out = acc_out_ref[:, pl.ds(at, shard)] + dot(chs[...], ys[:, pl.ds(at, shard)], 0, 0)
    cols = part_in.shape[1]
    for n, ref in enumerate(refs):
        rows = slice(n * ref.shape[0], (n + 1) * ref.shape[0])
        ref[:, 0:cols] = part_in[rows].astype(bf16)
        ref[:, cols:] = part_out[rows].astype(bf16)


def grad_kernel(chips, ids_ref, e0, e1, m0, m1, xs, silu, slope, hidden, wout, acc_in, acc_out, *refs):
    r3a_ref, r3b_ref, dgus, chs, ys, tab_ref = refs
    tok = ys.shape[0] // 2
    rep, expert = ids_ref[0], ids_ref[1]
    at_end = is_end(ids_ref[1], chips)
    ffn, experts = wout.shape[0], tab_ref.shape[1]

    width = ys.shape[1]

    @pl.when(at_end)
    def _():
        ys[0:tok, :] = unstack(e0, width)
        ys[tok:, :] = unstack(e1, width)

    @pl.when(jnp.logical_not(at_end))
    def _():
        ys[0:tok, :] = unstack(m0, width)
        ys[tok:, :] = unstack(m1, width)

    columns, first = [], width // 128 * tok
    for end, mid in ((e0, m0), (e1, m1)):
        table = jnp.where(at_end, end[first:, :].astype(f32), mid[first:, :].astype(f32))
        columns.append(gate_column(table, expert))
    gate = jnp.concatenate(columns, axis=0)
    back = dot(ys[...], wout[...], 1, 1)
    gate_grad = jnp.sum(hidden[...].astype(f32) * back, axis=1, keepdims=True)
    chs[...] = (hidden[...].astype(f32) * gate).astype(bf16)
    dh = back * gate
    dgus[:, :ffn] = (dh * slope[...]).astype(bf16)
    dgus[:, ffn:] = (dh * silu[...]).astype(bf16)
    for i in range(2):
        tab_ref[i] = gate_table(gate_grad[i * tok : (i + 1) * tok], experts, expert)
    half = r3a_ref.shape[0]
    shard_grads((r3a_ref, r3b_ref), acc_in, acc_out, xs, ys, dgus, chs, rep ^ 3, half)


def other_grads_kernel(ids_ref, xs, ys, dgus, chs, acc_in, acc_out, mine_ref, r1a_ref, r1b_ref, r2a_ref, r2b_ref):
    rep, half = ids_ref[0], r1a_ref.shape[0]
    args = (acc_in, acc_out, xs, ys, dgus, chs)
    shard_grads((r1a_ref, r1b_ref), *args, rep ^ 1, half)
    shard_grads((r2a_ref, r2b_ref), *args, rep ^ 2, half)
    shard_grads((mine_ref,), *args, rep, half)


def rows_kernel(dgus, win, tab_ref, keep_ref, give_ref):
    tok = dgus.shape[0] // 2
    row_grad = dot(dgus[...], win[...], 1, 1).astype(bf16)
    for i, out in enumerate((keep_ref, give_ref)):
        write_rows(out, row_grad[i * tok : (i + 1) * tok], tab_ref[i])


def finish_kernel(own_ref, t1a_ref, t1b_ref, t2a_ref, t2b_ref, min_ref, mout_ref, nin_ref, nout_ref):
    half = t1a_ref.shape[0]
    cols = min_ref.shape[2]
    for lo, one, two in ((0, t1a_ref, t2a_ref), (half, t1b_ref, t2b_ref)):
        rows = slice(lo, lo + half)
        total = own_ref[rows, :].astype(f32) + one[...].astype(f32) + two[...].astype(f32)
        old_in = momentum_decay * min_ref[0, rows, :].astype(f32)
        old_out = momentum_decay * mout_ref[0, rows, :].astype(f32)
        nin_ref[0, rows, :] = (old_in + total[:, :cols]).astype(bf16)
        nout_ref[0, rows, :] = (old_out + total[:, cols:]).astype(bf16)


def per_device_dense(*args):
    return dense_step(*args)


def dense_step(tokens, routes, gates, output_grad, w_in, w_out, momentum_in, momentum_out):
    tok, width = tokens.shape
    ffn, both_w = w_out.shape[1], w_in.shape[2]
    shard = w_in.shape[1]
    half = shard // 2
    cols = both_w + shard
    experts = lax.axis_size("expert")
    chips = experts // 2
    rep = lax.axis_index("rep")
    expert = lax.axis_index("expert")
    ids = jnp.stack([rep, expert]).astype(jnp.int32)

    def over_rep(value, bits):
        return lax.ppermute(value, "rep", [(i, i ^ bits) for i in range(4)])

    def over_chips(value, chip_pairs):
        pairs = [(2 * a + c, 2 * b + c) for a, b in chip_pairs for c in range(2)]
        return lax.ppermute(value, "expert", pairs)

    def partner(value):
        return lax.ppermute(value, "expert", [(i, i ^ 1) for i in range(experts)])

    to_far = [(z, z ^ 2) for z in range(chips)]
    to_near = [(z, z ^ 1) for z in range(chips)]
    to_cross = [(z, z ^ 3) for z in range(chips)]
    to_middle = [(1, 2), (2, 1)]
    to_ends = [(2, 3), (1, 0)]

    far_x = over_chips(tokens, to_far)
    w1in = over_rep(w_in, 1)
    w2in = over_rep(w_in, 2)
    near_x = over_chips(tokens, to_near)
    top = routes.shape[1]
    sources = [routes.T, gates.T, tokens, output_grad, w_in, w_out]
    own_x, own_y, own_in, own_out = call(
        stage_kernel,
        sources,
        [((tok, width), bf16), (stacked(width, tok, experts), bf16)]
        + [(w_in.shape, bf16), (w_out.shape, bf16)],
        [((top, tok), jnp.int32), ((top, tok), bf16), ((tok, width), bf16)]
        + [pltpu.SemaphoreType.DMA((len(sources),))],
        mib=4,
        far=len(sources),
    )
    far_y = over_chips(own_y, to_far)
    near_y = over_chips(own_y, to_near)
    w1out = over_rep(w_out, 1)
    w2out = over_rep(w_out, 2)
    middle_x = over_chips(tokens, to_middle)
    own_xp = partner(own_x)
    own_yp = partner(own_y)
    cut = shard * 3 // 4
    w3ina = over_rep(w1in[:, :cut], 2)
    ends_x = over_chips(far_x, to_ends)
    w3inb = over_rep(w2in[:, cut:], 1)
    w3out = over_rep(w2out, 1)
    far_xp = partner(far_x)
    near_xp = partner(near_x)
    middle_y = over_chips(own_y, to_middle)
    rows = 2 * tok
    block = ((tok + experts, width), bf16)
    flops = 5 * rows * width * both_w
    own_blocks = [own_x, own_xp, own_y, own_yp]
    keep, give_own, own_dgu, own_ch, win, wout = call(
        own_kernel,
        [ids, *own_blocks, own_in, w1in, w2in, w3ina, w3inb, own_out, w1out, w2out, w3out],
        [block, block, ((rows, both_w), bf16), ((rows, ffn), bf16)]
        + [((width, both_w), bf16), ((ffn, width), bf16)],
        mib=10,
        scalars=1,
        flops=flops,
    )
    ends_y = over_chips(far_y, to_ends)
    far_yp = partner(far_y)
    near_yp = partner(near_y)
    middle_xp = partner(middle_x)
    ends_xp = partner(ends_x)
    got = partner(give_own)
    home_own = (keep.astype(f32) + got.astype(f32)).astype(bf16)
    more_xs, *early = call(
        early_kernel,
        [near_x, near_xp, far_x, far_xp, win],
        [((2 * rows, width), bf16), ((2 * rows, ffn), f32), ((2 * rows, ffn), f32), ((2 * rows, ffn), bf16)],
        mib=6,
        flops=2 * flops // 5 * 2,
    )
    keep, give, *more = call(
        rest_kernel,
        [ids, near_y, near_yp, far_y, far_yp, *early, win, wout],
        [((2, tok + experts, width), bf16)] * 2
        + [((2 * rows, width), bf16), ((2 * rows, both_w), bf16), ((2 * rows, ffn), bf16)],
        mib=8,
        scalars=1,
        flops=flops,
    )
    acc_in, acc_out = call(
        sum_kernel,
        [*own_blocks, own_dgu, own_ch, more_xs, *more],
        [((width, both_w), f32), ((ffn, width), f32)],
        [((3 * rows, n), bf16) for n in (width, width, both_w, ffn)],
        mib=16,
        flops=2 * flops,
    )
    got = partner(give)
    home_near, home_far = ((keep[i].astype(f32) + got[i].astype(f32)).astype(bf16) for i in range(2))
    xs, silu, slope, hidden = call(
        functools.partial(forward_kernel, chips),
        [ids, ends_x, ends_xp, middle_x, middle_xp, win],
        [((rows, width), bf16), ((rows, ffn), f32), ((rows, ffn), f32), ((rows, ffn), bf16)],
        scalars=1,
        flops=2 * rows * width * both_w,
    )
    middle_yp = partner(middle_y)
    ends_yp = partner(ends_y)
    home_near = over_chips(home_near, to_near)
    home_far = over_chips(home_far, to_far)
    r3a, r3b, dgus, chs, ys, table = call(
        functools.partial(grad_kernel, chips),
        [ids, ends_y, ends_yp, middle_y, middle_yp, xs, silu, slope, hidden, wout]
        + [acc_in, acc_out],
        [((half, cols), bf16)] * 2
        + [((rows, both_w), bf16), ((rows, ffn), bf16), ((rows, width), bf16), ((2, experts, tok), f32)],
        mib=8,
        scalars=1,
        flops=rows * width * both_w * 2,
    )
    s3a = over_rep(r3a, 2)
    s3b = over_rep(r3b, 1)
    mine, r1a, r1b, r2a, r2b = call(
        other_grads_kernel,
        [ids, xs, ys, dgus, chs, acc_in, acc_out],
        [((shard, cols), bf16)] + [((half, cols), bf16)] * 4,
        mib=8,
        scalars=1,
        flops=2 * rows * width * both_w,
    )
    keep2, give2 = call(rows_kernel, [dgus, win, table], [block, block])
    got2 = partner(give2)
    t2a = over_rep(r2a, 2)
    t1b = over_rep(r1b, 1)
    last = (keep2.astype(f32) + got2.astype(f32)).astype(bf16)
    home_cross = over_chips(last, to_cross)
    t1a = over_rep((r1a.astype(f32) + s3a.astype(f32)).astype(bf16), 1)
    t2b = over_rep((r2b.astype(f32) + s3b.astype(f32)).astype(bf16), 2)
    parts = (home_own, home_near, home_far, home_cross)
    token_grad = sum(p[:tok].astype(f32) for p in parts).astype(bf16)
    table = sum(p[tok:, :tok].astype(f32) for p in parts)
    picked = routes.T[:, None, :] == jnp.arange(experts, dtype=jnp.int32)[None, :, None]
    gate_grad = jnp.sum(jnp.where(picked, table[None], 0.0), axis=1).astype(bf16).T
    new_in, new_out = call(
        finish_kernel,
        [mine, t1a, t1b, t2a, t2b, momentum_in, momentum_out],
        [(momentum_in.shape, bf16), (momentum_out.shape, bf16)],
    )
    return token_grad, gate_grad, new_in, new_out


def slot_positions(routes, experts):
    flat_routes = routes.reshape(-1)
    one_hot = (flat_routes[:, None] == jnp.arange(experts, dtype=jnp.int32)[None, :]).astype(
        jnp.int32
    )
    earlier = jnp.cumsum(one_hot, axis=0) - one_hot
    return jnp.sum(earlier * one_hot, axis=1)


def forward_pass(x_rows, weight_in, weight_out):
    width_ffn = weight_out.shape[0]
    both = jnp.dot(x_rows, weight_in, preferred_element_type=jnp.float32)
    gate_pre = both[:, :width_ffn]
    up_part = both[:, width_ffn:]
    silu_gate = jax.nn.silu(gate_pre)
    hidden = (silu_gate * up_part).astype(jnp.bfloat16)
    expert_out = jnp.dot(hidden, weight_out, preferred_element_type=jnp.float32)
    return (gate_pre, up_part, silu_gate, hidden, expert_out)


def per_device_sparse(tokens, routes, gates, output_grad, w_in, w_out, momentum_in, momentum_out):
    tok_dev, width = tokens.shape
    top_count = routes.shape[1]
    senders = lax.axis_size("expert")
    local_count = w_in.shape[0]
    experts = senders * local_count
    capacity = max(2, min(tok_dev, 5 * tok_dev * top_count // (4 * experts)))
    slot_count = experts * capacity
    target = routes.reshape(-1) * capacity + slot_positions(routes, experts)
    token_ids = jnp.repeat(jnp.arange(tok_dev, dtype=jnp.int32), top_count)
    source_row = jnp.full((slot_count,), tok_dev, jnp.int32).at[target].set(token_ids)
    slot_gate = jnp.zeros((slot_count,), jnp.bfloat16).at[target].set(gates.reshape(-1))
    zero_row = jnp.zeros((1, width), jnp.bfloat16)
    sent_tokens = jnp.concatenate([tokens, zero_row], axis=0)[source_row].reshape(
        experts, capacity, width
    )
    sent_grads = jnp.concatenate([output_grad, zero_row], axis=0)[source_row].reshape(
        experts, capacity, width
    )
    sent_gate = slot_gate.reshape(experts, capacity)
    whole_in, whole_out = (
        lax.all_gather(w_in, "rep", axis=1, tiled=True),
        lax.all_gather(w_out, "rep", axis=2, tiled=True),
    )

    def local_rows(received, expert):
        shaped = received.reshape((senders, local_count) + received.shape[1:])
        return shaped[:, expert].reshape((senders * capacity,) + received.shape[2:])

    got_tokens, got_grads, got_gate = (
        lax.all_to_all(sent_tokens, "expert", split_axis=0, concat_axis=0, tiled=True),
        lax.all_to_all(sent_grads, "expert", split_axis=0, concat_axis=0, tiled=True),
        lax.all_to_all(sent_gate, "expert", split_axis=0, concat_axis=0, tiled=True),
    )
    forward = [forward_pass(local_rows(got_tokens, 0), whole_in[0], whole_out[0])]
    expert = 0
    gate_pre, up_part, silu_gate, hidden, expert_out = forward[expert]
    dy_rows = local_rows(got_grads, expert)
    gate_grad = jnp.sum(expert_out * dy_rows.astype(jnp.float32), axis=1).astype(jnp.bfloat16)
    scaled = (
        local_rows(got_gate, expert).astype(jnp.float32)[:, None] * dy_rows.astype(jnp.float32)
    ).astype(jnp.bfloat16)
    scaled_rows = [scaled]
    gate_rows = [gate_grad]
    parts_out = [
        lax.dot_general(
            hidden, scaled, (((0,), (0,)), ((), ())), preferred_element_type=jnp.float32
        )
    ]
    grad_out_all = jnp.stack(parts_out)
    summed_out = lax.psum_scatter(
        grad_out_all.astype(jnp.bfloat16), "rep", scatter_dimension=2, tiled=True
    ).astype(jnp.float32)
    expert = 0
    gate_pre, up_part, silu_gate, hidden, expert_out = forward[expert]
    hidden_grad = lax.dot_general(
        scaled_rows[expert],
        whole_out[expert],
        (((1,), (1,)), ((), ())),
        preferred_element_type=jnp.float32,
    )
    sigma = jax.nn.sigmoid(gate_pre)
    dgu = jnp.concatenate(
        [hidden_grad * up_part * sigma * (1.0 + gate_pre * (1.0 - sigma)), hidden_grad * silu_gate],
        axis=1,
    ).astype(jnp.bfloat16)
    row_grad = lax.dot_general(
        dgu, whole_in[expert], (((1,), (1,)), ((), ())), preferred_element_type=jnp.float32
    ).astype(jnp.bfloat16)
    row_grads = row_grad.reshape(senders, 1, capacity, width)
    parts_in = [
        lax.dot_general(
            local_rows(got_tokens, expert),
            dgu,
            (((0,), (0,)), ((), ())),
            preferred_element_type=jnp.float32,
        )
    ]
    grad_in_all = jnp.stack(parts_in)
    back_send = row_grads.reshape(experts, capacity, width)
    gate_send = jnp.stack([item.reshape(senders, capacity) for item in gate_rows], axis=1).reshape(
        experts, capacity
    )
    back_rows, back_gate = (
        lax.all_to_all(back_send, "expert", split_axis=0, concat_axis=0, tiled=True),
        lax.all_to_all(gate_send, "expert", split_axis=0, concat_axis=0, tiled=True),
    )
    picked = back_rows.reshape(slot_count, width)[target].reshape(tok_dev, top_count, width)
    token_grad = jnp.sum(picked.astype(jnp.float32), axis=1).astype(jnp.bfloat16)
    gate_grad_out = back_gate.reshape(-1)[target].reshape(tok_dev, top_count)
    summed_in = lax.psum_scatter(
        grad_in_all.astype(jnp.bfloat16), "rep", scatter_dimension=1, tiled=True
    ).astype(jnp.float32)
    new_momentum_in = (momentum_decay * momentum_in.astype(jnp.float32) + summed_in).astype(
        jnp.bfloat16
    )
    new_momentum_out = (momentum_decay * momentum_out.astype(jnp.float32) + summed_out).astype(
        jnp.bfloat16
    )
    return (token_grad, gate_grad_out, new_momentum_in, new_momentum_out)


def solution(mesh):
    in_specs = (
        P(("rep", "expert"), None),
        P(("rep", "expert"), None),
        P(("rep", "expert"), None),
        P(("rep", "expert"), None),
        P("expert", "rep", None),
        P("expert", None, "rep"),
        P("expert", "rep", None),
        P("expert", None, "rep"),
    )
    out_specs = (
        P(("rep", "expert"), None),
        P(("rep", "expert"), None),
        P("expert", "rep", None),
        P("expert", None, "rep"),
    )

    small = mesh.shape["expert"] == 8 and mesh.shape["rep"] == 4

    def per_device(*args):
        tok, width = args[0].shape
        w_in, w_out = args[4], args[5]
        lanes = (tok, w_in.shape[1], w_out.shape[1], w_out.shape[2], w_in.shape[2])
        fits = small and tok == 128 and width >= tok and all(n % 128 == 0 for n in lanes)
        dense = fits and w_in.shape[0] == 1 and w_in.shape[1] == w_out.shape[2] == w_out.shape[1]
        return (per_device_dense if dense else per_device_sparse)(*args)

    return jax.shard_map(
        per_device, mesh=mesh, in_specs=in_specs, out_specs=out_specs, check_vma=False
    )
```

```python
import jax
import jax.numpy as jnp
from jax import lax
from jax.experimental import pallas as pl
from jax.experimental.pallas import tpu as pltpu
from jax.sharding import PartitionSpec as P


momentum_decay = 0.9
bf16 = jnp.bfloat16
f32 = jnp.float32
MIB = 1024 * 1024


def dot(a, b, left, right):
    return lax.dot_general(a, b, (((left,), (right,)), ((), ())), preferred_element_type=f32)


def call(kernel, operands, outs, scratch=(), mib=8, scalars=0, flops=0, far=0):
    specs = [pl.BlockSpec(memory_space=pltpu.SMEM)] * scalars
    specs += [pl.BlockSpec(memory_space=pltpu.VMEM)] * (len(operands) - scalars - far)
    specs += [pl.BlockSpec(memory_space=pltpu.HBM)] * far
    return pl.pallas_call(
        kernel,
        out_shape=[jax.ShapeDtypeStruct(shape, dtype) for shape, dtype in outs],
        in_specs=specs,
        out_specs=[pl.BlockSpec(memory_space=pltpu.VMEM)] * len(outs),
        scratch_shapes=[pltpu.VMEM(*item) if isinstance(item, tuple) else item for item in scratch],
        compiler_params=pltpu.CompilerParams(vmem_limit_bytes=mib * MIB),
        cost_estimate=pl.CostEstimate(flops=flops, bytes_accessed=4 * MIB, transcendentals=0),
    )(*operands)


def stage_kernel(routes_hbm, gates_hbm, x_hbm, y_hbm, win_hbm, wout_hbm, *refs):
    x_ref, block_ref, win_ref, wout_ref, routes_ref, gates_ref, y_ref, sems = refs
    tok, width = y_ref.shape
    moves = (
        (routes_hbm, routes_ref),
        (gates_hbm, gates_ref),
        (y_hbm, y_ref),
        (x_hbm, x_ref),
        (win_hbm, win_ref),
        (wout_hbm, wout_ref),
    )
    copies = [pltpu.make_async_copy(src, dst, sems.at[i]) for i, (src, dst) in enumerate(moves)]
    for copy in copies:
        copy.start()
    copies[0].wait()
    copies[1].wait()
    first = width // 128 * tok
    experts = block_ref.shape[0] - first
    ids = lax.broadcasted_iota(jnp.int32, (experts, tok), 0)
    dense = jnp.zeros((experts, tok), f32)
    for k in range(routes_ref.shape[0]):
        gate = gates_ref[k : k + 1, :].astype(f32)
        dense = dense + jnp.where(ids == routes_ref[k : k + 1, :], gate, 0.0)
    block_ref[first:, :] = dense.astype(bf16)
    copies[2].wait()
    for j in range(width // 128):
        block_ref[j * tok : (j + 1) * tok, :] = y_ref[:, j * 128 : (j + 1) * 128]
    for copy in copies[3:]:
        copy.wait()


def stacked(width, tok, experts):
    return (width // 128 * tok + experts, 128)


def unstack(ref, width):
    tok = 128
    return jnp.concatenate([ref[j * tok : (j + 1) * tok, :] for j in range(width // 128)], axis=1)


def gate_column(table, expert):
    pick = lax.broadcasted_iota(jnp.int32, table.shape, 0) == expert
    return jnp.sum(jnp.where(pick, table.astype(f32), 0.0).T, axis=1, keepdims=True)


def gate_table(column, experts, expert):
    spread = jnp.broadcast_to(column, (column.shape[0], experts)).T
    pick = lax.broadcasted_iota(jnp.int32, spread.shape, 0) == expert
    return jnp.where(pick, spread, 0.0)


def write_rows(out, row_grad, table):
    tok = row_grad.shape[0]
    out[0:tok, :] = row_grad
    tail = jnp.zeros((table.shape[0], out.shape[1] - tok), f32)
    out[tok:, :] = jnp.concatenate([table, tail], axis=1).astype(bf16)


def activations(both):
    ffn = both.shape[1] // 2
    g, u = both[:, :ffn], both[:, ffn:]
    s = 1.0 / (1.0 + jnp.exp(-g))
    silu = g * s
    hidden = (silu * u).astype(bf16)
    return silu, u * s * (1.0 + g * (1.0 - s)), hidden


def back_step(tables, expert, y, acts, win, wout, keep_ref, give_ref, dgu_ref, ch_ref):
    silu, slope, hidden = acts
    tok, ffn, experts = y.shape[0] // 2, wout.shape[0], tables[0].shape[0]
    gate = jnp.concatenate([gate_column(table, expert) for table in tables], axis=0)
    back = dot(y, wout[...], 1, 1)
    gate_grad = jnp.sum(hidden.astype(f32) * back, axis=1, keepdims=True)
    ch_ref[...] = (hidden.astype(f32) * gate).astype(bf16)
    dh = back * gate
    dgu_ref[:, :ffn] = (dh * slope).astype(bf16)
    dgu_ref[:, ffn:] = (dh * silu).astype(bf16)
    row_grad = dot(dgu_ref[...], win[...], 1, 1).astype(bf16)
    for i, out in enumerate((keep_ref, give_ref)):
        part = slice(i * tok, (i + 1) * tok)
        write_rows(out, row_grad[part], gate_table(gate_grad[part], experts, expert))


def own_kernel(ids_ref, x0, x1, y0, y1, *refs):
    in_pieces, out_pieces, refs = refs[0:5], refs[5:9], refs[9:]
    keep_ref, give_ref, dgu_ref, ch_ref, win, wout = refs
    rep, expert = ids_ref[0], ids_ref[1]
    shard, (tok, width) = wout.shape[1] // 4, x0.shape
    cut = in_pieces[3].shape[1]
    for j in range(4):
        at = pl.multiple_of((rep ^ j) * shard, 128)
        wout[:, pl.ds(at, shard)] = out_pieces[j][0]
        if j < 3:
            win[pl.ds(at, shard), :] = in_pieces[j][0]
        else:
            win[pl.ds(at, cut), :] = in_pieces[3][0]
            win[pl.ds(at + cut, shard - cut), :] = in_pieces[4][0]
    tables = [ref[width // 128 * tok :, :] for ref in (y0, y1)]
    x = jnp.concatenate([x0[...], x1[...]], axis=0)
    y = jnp.concatenate([unstack(y0, width), unstack(y1, width)], axis=0)
    acts = activations(dot(x, win[...], 1, 0))
    back_step(tables, expert, y, acts, win, wout, keep_ref, give_ref, dgu_ref, ch_ref)


def early_kernel(n0, n1, f0, f1, win, xs, silu_ref, slope_ref, hidden_ref):
    tok = n0.shape[0]
    for n, ref in enumerate((n0, n1, f0, f1)):
        xs[n * tok : (n + 1) * tok, :] = ref[...]
    silu_ref[...], slope_ref[...], hidden_ref[...] = activations(dot(xs[...], win[...], 1, 0))


def rest_kernel(ids_ref, *refs):
    blocks, (silu, slope, hidden, win, wout), refs = refs[0:4], refs[4:9], refs[9:]
    keep_ref, give_ref, ys, dgus, chs = refs
    rows, width = ys.shape[0] // 2, ys.shape[1]
    tok = rows // 2
    for n in range(2):
        part, pair = slice(n * rows, (n + 1) * rows), blocks[2 * n : 2 * n + 2]
        for i, ref in enumerate(pair):
            ys[n * rows + i * tok : n * rows + (i + 1) * tok, :] = unstack(ref, width)
        tables = [ref[width // 128 * tok :, :] for ref in pair]
        acts = (silu[part, :], slope[part, :], hidden[part, :])
        outs = (keep_ref.at[n], give_ref.at[n], dgus.at[part], chs.at[part])
        back_step(tables, ids_ref[1], ys[part, :], acts, win, wout, *outs)


def sum_kernel(x0, x1, y0, y1, own_dgu, own_ch, more_xs, more_ys, more_dgu, more_ch, *refs):
    acc_in_ref, acc_out_ref, xs, ys, dgus, chs = refs
    tok, width = x0.shape
    rows = 2 * tok
    for i, (x, y) in enumerate(((x0, y0), (x1, y1))):
        xs[i * tok : (i + 1) * tok, :] = x[...]
        ys[i * tok : (i + 1) * tok, :] = unstack(y, width)
    for whole, first, more in ((dgus, own_dgu, more_dgu), (chs, own_ch, more_ch)):
        whole[0:rows, :] = first[...]
        whole[rows:, :] = more[...]
    xs[rows:, :] = more_xs[...]
    ys[rows:, :] = more_ys[...]
    acc_in_ref[...] = dot(xs[...], dgus[...], 0, 0)
    acc_out_ref[...] = dot(chs[...], ys[...], 0, 0)


def forward_kernel(x0, x1, win, xs, silu_ref, slope_ref, hidden_ref):
    tok = x0.shape[0]
    xs[0:tok, :] = x0[...]
    xs[tok:, :] = x1[...]
    silu_ref[...], slope_ref[...], hidden_ref[...] = activations(dot(xs[...], win[...], 1, 0))


def shard_grads(refs, acc_in_ref, acc_out_ref, xs, ys, dgus, chs, index):
    shard = sum(ref.shape[0] for ref in refs)
    at = pl.multiple_of(index * shard, 128)
    part_in = acc_in_ref[pl.ds(at, shard), :] + dot(xs[:, pl.ds(at, shard)], dgus[...], 0, 0)
    part_out = acc_out_ref[:, pl.ds(at, shard)] + dot(chs[...], ys[:, pl.ds(at, shard)], 0, 0)
    cols = part_in.shape[1]
    at = 0
    for ref in refs:
        rows = slice(at, at + ref.shape[0])
        ref[:, 0:cols] = part_in[rows].astype(bf16)
        ref[:, cols:] = part_out[rows].astype(bf16)
        at = rows.stop


def grad_kernel(ids_ref, y0, y1, xs, silu, slope, hidden, wout, acc_in, acc_out, *refs):
    r3a_ref, r3b_ref, dgus, chs, ys, tab_ref = refs
    rep, expert = ids_ref[0], ids_ref[1]
    tok, width = ys.shape[0] // 2, ys.shape[1]
    ffn, experts = wout.shape[0], tab_ref.shape[1]
    ys[0:tok, :] = unstack(y0, width)
    ys[tok:, :] = unstack(y1, width)
    first = width // 128 * tok
    gate = jnp.concatenate([gate_column(ref[first:, :], expert) for ref in (y0, y1)], axis=0)
    back = dot(ys[...], wout[...], 1, 1)
    gate_grad = jnp.sum(hidden[...].astype(f32) * back, axis=1, keepdims=True)
    chs[...] = (hidden[...].astype(f32) * gate).astype(bf16)
    dh = back * gate
    dgus[:, :ffn] = (dh * slope[...]).astype(bf16)
    dgus[:, ffn:] = (dh * silu[...]).astype(bf16)
    for i in range(2):
        tab_ref[i] = gate_table(gate_grad[i * tok : (i + 1) * tok], experts, expert)
    shard_grads((r3a_ref, r3b_ref), acc_in, acc_out, xs, ys, dgus, chs, rep ^ 3)


def other_grads_kernel(ids_ref, xs, ys, dgus, chs, acc_in, acc_out, mine_ref, r1a_ref, r1b_ref, r2a_ref, r2b_ref):
    rep = ids_ref[0]
    args = (acc_in, acc_out, xs, ys, dgus, chs)
    shard_grads((r1a_ref, r1b_ref), *args, rep ^ 1)
    shard_grads((r2a_ref, r2b_ref), *args, rep ^ 2)
    shard_grads((mine_ref,), *args, rep)


def rows_kernel(dgus, win, tab_ref, keep_ref, give_ref):
    tok = dgus.shape[0] // 2
    row_grad = dot(dgus[...], win[...], 1, 1).astype(bf16)
    for i, out in enumerate((keep_ref, give_ref)):
        write_rows(out, row_grad[i * tok : (i + 1) * tok], tab_ref[i])


def mix_kernel(own_ref, t1b_ref, t2a_ref, min_ref, mout_ref, base_ref):
    cut, cols = t2a_ref.shape[0], min_ref.shape[2]
    for rows, part in ((slice(0, cut), t2a_ref), (slice(cut, own_ref.shape[0]), t1b_ref)):
        total = own_ref[rows, :].astype(f32) + part[...].astype(f32)
        base_ref[rows, 0:cols] = total[:, :cols] + momentum_decay * min_ref[0, rows, :].astype(f32)
        base_ref[rows, cols:] = total[:, cols:] + momentum_decay * mout_ref[0, rows, :].astype(f32)


def finish_kernel(base_ref, t1a_ref, t2b_ref, nin_ref, nout_ref):
    cut, cols = t1a_ref.shape[0], nin_ref.shape[2]
    for rows, part in ((slice(0, cut), t1a_ref), (slice(cut, base_ref.shape[0]), t2b_ref)):
        total = (base_ref[rows, :] + part[...].astype(f32)).astype(bf16)
        nin_ref[0, rows, :] = total[:, :cols]
        nout_ref[0, rows, :] = total[:, cols:]


def per_device_dense(*args):
    return dense_step(*args)


def dense_step(tokens, routes, gates, output_grad, w_in, w_out, momentum_in, momentum_out):
    tok, width = tokens.shape
    ffn, both_w = w_out.shape[1], w_in.shape[2]
    shard = w_in.shape[1]
    cols = both_w + shard
    experts = lax.axis_size("expert")
    chips = experts // 2
    rep = lax.axis_index("rep")
    expert = lax.axis_index("expert")
    ids = jnp.stack([rep, expert]).astype(jnp.int32)

    def over_rep(value, bits):
        return lax.ppermute(value, "rep", [(i, i ^ bits) for i in range(4)])

    def over_chips(value, chip_pairs):
        pairs = [(2 * a + c, 2 * b + c) for a, b in chip_pairs for c in range(2)]
        return lax.ppermute(value, "expert", pairs)

    def partner(value):
        return lax.ppermute(value, "expert", [(i, i ^ 1) for i in range(experts)])

    to_far = [(z, z ^ 2) for z in range(chips)]
    to_near = [(z, z ^ 1) for z in range(chips)]
    to_cross = [(z, z ^ 3) for z in range(chips)]
    to_middle = [(1, 2), (2, 1)]
    to_ends = [(2, 3), (1, 0)]

    far_x = over_chips(tokens, to_far)
    w1in = over_rep(w_in, 1)
    w2in = over_rep(w_in, 2)
    near_x = over_chips(tokens, to_near)
    top = routes.shape[1]
    sources = [routes.T, gates.T, tokens, output_grad, w_in, w_out]
    own_x, own_y, own_in, own_out = call(
        stage_kernel,
        sources,
        [((tok, width), bf16), (stacked(width, tok, experts), bf16)]
        + [(w_in.shape, bf16), (w_out.shape, bf16)],
        [((top, tok), jnp.int32), ((top, tok), bf16), ((tok, width), bf16)]
        + [pltpu.SemaphoreType.DMA((len(sources),))],
        mib=4,
        far=len(sources),
    )
    far_y = over_chips(own_y, to_far)
    near_y = over_chips(own_y, to_near)
    w1out = over_rep(w_out, 1)
    w2out = over_rep(w_out, 2)
    middle_x = over_chips(tokens, to_middle)
    own_xp = partner(own_x)
    own_yp = partner(own_y)
    cut = shard * 3 // 4
    w3ina = over_rep(w1in[:, :cut], 2)
    ends_x = over_chips(far_x, to_ends)
    w3inb = over_rep(w2in[:, cut:], 1)
    w3out = over_rep(w2out, 1)
    far_xp = partner(far_x)
    near_xp = partner(near_x)
    middle_y = over_chips(own_y, to_middle)
    rows = 2 * tok
    block = ((tok + experts, width), bf16)
    flops = 5 * rows * width * both_w
    own_blocks = [own_x, own_xp, own_y, own_yp]
    keep, give_own, own_dgu, own_ch, win, wout = call(
        own_kernel,
        [ids, *own_blocks, own_in, w1in, w2in, w3ina, w3inb, own_out, w1out, w2out, w3out],
        [block, block, ((rows, both_w), bf16), ((rows, ffn), bf16)]
        + [((width, both_w), bf16), ((ffn, width), bf16)],
        mib=10,
        scalars=1,
        flops=flops,
    )
    ends_y = over_chips(far_y, to_ends)
    far_yp = partner(far_y)
    near_yp = partner(near_y)
    got = partner(give_own)
    home_own = (keep.astype(f32) + got.astype(f32)).astype(bf16)
    more_xs, *early = call(
        early_kernel,
        [near_x, near_xp, far_x, far_xp, win],
        [((2 * rows, width), bf16), ((2 * rows, ffn), f32), ((2 * rows, ffn), f32), ((2 * rows, ffn), bf16)],
        mib=6,
        flops=2 * flops // 5 * 2,
    )
    keep, give, *more = call(
        rest_kernel,
        [ids, near_y, near_yp, far_y, far_yp, *early, win, wout],
        [((2, tok + experts, width), bf16)] * 2
        + [((2 * rows, width), bf16), ((2 * rows, both_w), bf16), ((2 * rows, ffn), bf16)],
        mib=8,
        scalars=1,
        flops=flops,
    )
    acc_in, acc_out = call(
        sum_kernel,
        [*own_blocks, own_dgu, own_ch, more_xs, *more],
        [((width, both_w), f32), ((ffn, width), f32)],
        [((3 * rows, n), bf16) for n in (width, width, both_w, ffn)],
        mib=16,
        flops=2 * flops,
    )
    got = partner(give)
    home_near, home_far = ((keep[i].astype(f32) + got[i].astype(f32)).astype(bf16) for i in range(2))
    cross_x = ends_x + middle_x
    cross_xp = partner(cross_x)
    xs, silu, slope, hidden = call(
        forward_kernel,
        [cross_x, cross_xp, win],
        [((rows, width), bf16), ((rows, ffn), f32), ((rows, ffn), f32), ((rows, ffn), bf16)],
        flops=2 * rows * width * both_w,
    )
    cross_y = ends_y + middle_y
    cross_yp = partner(cross_y)
    home_near = over_chips(home_near, to_near)
    home_far = over_chips(home_far, to_far)
    part_a = shard * 13 // 24 // 16 * 16
    part_b = shard - part_a
    r3a, r3b, dgus, chs, ys, table = call(
        grad_kernel,
        [ids, cross_y, cross_yp, xs, silu, slope, hidden, wout]
        + [acc_in, acc_out],
        [((part_a, cols), bf16), ((part_b, cols), bf16)]
        + [((rows, both_w), bf16), ((rows, ffn), bf16), ((rows, width), bf16), ((2, experts, tok), f32)],
        mib=8,
        scalars=1,
        flops=rows * width * both_w * 2,
    )
    s3a = over_rep(r3a, 2)
    s3b = over_rep(r3b, 1)
    mine, r1a, r1b, r2a, r2b = call(
        other_grads_kernel,
        [ids, xs, ys, dgus, chs, acc_in, acc_out],
        [((shard, cols), bf16)] + [((part_a, cols), bf16), ((part_b, cols), bf16)] * 2,
        mib=8,
        scalars=1,
        flops=2 * rows * width * both_w,
    )
    keep2, give2 = call(rows_kernel, [dgus, win, table], [block, block])
    got2 = partner(give2)
    t2a = over_rep(r2a, 2)
    t1b = over_rep(r1b, 1)
    last = (keep2.astype(f32) + got2.astype(f32)).astype(bf16)
    home_cross = over_chips(last, to_cross)
    t1a = over_rep((r1a.astype(f32) + s3a.astype(f32)).astype(bf16), 1)
    t2b = over_rep((r2b.astype(f32) + s3b.astype(f32)).astype(bf16), 2)
    parts = (home_own, home_near, home_far, home_cross)
    token_grad = sum(p[:tok].astype(f32) for p in parts).astype(bf16)
    table = sum(p[tok:, :tok].astype(f32) for p in parts)
    picked = routes.T[:, None, :] == jnp.arange(experts, dtype=jnp.int32)[None, :, None]
    gate_grad = jnp.sum(jnp.where(picked, table[None], 0.0), axis=1).astype(bf16).T
    (base,) = call(mix_kernel, [mine, t1b, t2a, momentum_in, momentum_out], [((shard, cols), f32)])
    new_in, new_out = call(
        finish_kernel, [base, t1a, t2b], [(momentum_in.shape, bf16), (momentum_out.shape, bf16)]
    )
    return token_grad, gate_grad, new_in, new_out


def slot_positions(routes, experts):
    flat_routes = routes.reshape(-1)
    one_hot = (flat_routes[:, None] == jnp.arange(experts, dtype=jnp.int32)[None, :]).astype(
        jnp.int32
    )
    earlier = jnp.cumsum(one_hot, axis=0) - one_hot
    return jnp.sum(earlier * one_hot, axis=1)


def forward_pass(x_rows, weight_in, weight_out):
    width_ffn = weight_out.shape[0]
    both = jnp.dot(x_rows, weight_in, preferred_element_type=jnp.float32)
    gate_pre = both[:, :width_ffn]
    up_part = both[:, width_ffn:]
    silu_gate = jax.nn.silu(gate_pre)
    hidden = (silu_gate * up_part).astype(jnp.bfloat16)
    expert_out = jnp.dot(hidden, weight_out, preferred_element_type=jnp.float32)
    return (gate_pre, up_part, silu_gate, hidden, expert_out)


def per_device_sparse(tokens, routes, gates, output_grad, w_in, w_out, momentum_in, momentum_out):
    tok_dev, width = tokens.shape
    top_count = routes.shape[1]
    senders = lax.axis_size("expert")
    local_count = w_in.shape[0]
    experts = senders * local_count
    capacity = max(2, min(tok_dev, 5 * tok_dev * top_count // (4 * experts)))
    slot_count = experts * capacity
    target = routes.reshape(-1) * capacity + slot_positions(routes, experts)
    token_ids = jnp.repeat(jnp.arange(tok_dev, dtype=jnp.int32), top_count)
    source_row = jnp.full((slot_count,), tok_dev, jnp.int32).at[target].set(token_ids)
    slot_gate = jnp.zeros((slot_count,), jnp.bfloat16).at[target].set(gates.reshape(-1))
    zero_row = jnp.zeros((1, width), jnp.bfloat16)
    sent_tokens = jnp.concatenate([tokens, zero_row], axis=0)[source_row].reshape(
        experts, capacity, width
    )
    sent_grads = jnp.concatenate([output_grad, zero_row], axis=0)[source_row].reshape(
        experts, capacity, width
    )
    sent_gate = slot_gate.reshape(experts, capacity)
    whole_in, whole_out = (
        lax.all_gather(w_in, "rep", axis=1, tiled=True),
        lax.all_gather(w_out, "rep", axis=2, tiled=True),
    )

    def local_rows(received, expert):
        shaped = received.reshape((senders, local_count) + received.shape[1:])
        return shaped[:, expert].reshape((senders * capacity,) + received.shape[2:])

    got_tokens, got_grads, got_gate = (
        lax.all_to_all(sent_tokens, "expert", split_axis=0, concat_axis=0, tiled=True),
        lax.all_to_all(sent_grads, "expert", split_axis=0, concat_axis=0, tiled=True),
        lax.all_to_all(sent_gate, "expert", split_axis=0, concat_axis=0, tiled=True),
    )
    forward = [forward_pass(local_rows(got_tokens, 0), whole_in[0], whole_out[0])]
    expert = 0
    gate_pre, up_part, silu_gate, hidden, expert_out = forward[expert]
    dy_rows = local_rows(got_grads, expert)
    gate_grad = jnp.sum(expert_out * dy_rows.astype(jnp.float32), axis=1).astype(jnp.bfloat16)
    scaled = (
        local_rows(got_gate, expert).astype(jnp.float32)[:, None] * dy_rows.astype(jnp.float32)
    ).astype(jnp.bfloat16)
    scaled_rows = [scaled]
    gate_rows = [gate_grad]
    parts_out = [
        lax.dot_general(
            hidden, scaled, (((0,), (0,)), ((), ())), preferred_element_type=jnp.float32
        )
    ]
    grad_out_all = jnp.stack(parts_out)
    summed_out = lax.psum_scatter(
        grad_out_all.astype(jnp.bfloat16), "rep", scatter_dimension=2, tiled=True
    ).astype(jnp.float32)
    expert = 0
    gate_pre, up_part, silu_gate, hidden, expert_out = forward[expert]
    hidden_grad = lax.dot_general(
        scaled_rows[expert],
        whole_out[expert],
        (((1,), (1,)), ((), ())),
        preferred_element_type=jnp.float32,
    )
    sigma = jax.nn.sigmoid(gate_pre)
    dgu = jnp.concatenate(
        [hidden_grad * up_part * sigma * (1.0 + gate_pre * (1.0 - sigma)), hidden_grad * silu_gate],
        axis=1,
    ).astype(jnp.bfloat16)
    row_grad = lax.dot_general(
        dgu, whole_in[expert], (((1,), (1,)), ((), ())), preferred_element_type=jnp.float32
    ).astype(jnp.bfloat16)
    row_grads = row_grad.reshape(senders, 1, capacity, width)
    parts_in = [
        lax.dot_general(
            local_rows(got_tokens, expert),
            dgu,
            (((0,), (0,)), ((), ())),
            preferred_element_type=jnp.float32,
        )
    ]
    grad_in_all = jnp.stack(parts_in)
    back_send = row_grads.reshape(experts, capacity, width)
    gate_send = jnp.stack([item.reshape(senders, capacity) for item in gate_rows], axis=1).reshape(
        experts, capacity
    )
    back_rows, back_gate = (
        lax.all_to_all(back_send, "expert", split_axis=0, concat_axis=0, tiled=True),
        lax.all_to_all(gate_send, "expert", split_axis=0, concat_axis=0, tiled=True),
    )
    picked = back_rows.reshape(slot_count, width)[target].reshape(tok_dev, top_count, width)
    token_grad = jnp.sum(picked.astype(jnp.float32), axis=1).astype(jnp.bfloat16)
    gate_grad_out = back_gate.reshape(-1)[target].reshape(tok_dev, top_count)
    summed_in = lax.psum_scatter(
        grad_in_all.astype(jnp.bfloat16), "rep", scatter_dimension=1, tiled=True
    ).astype(jnp.float32)
    new_momentum_in = (momentum_decay * momentum_in.astype(jnp.float32) + summed_in).astype(
        jnp.bfloat16
    )
    new_momentum_out = (momentum_decay * momentum_out.astype(jnp.float32) + summed_out).astype(
        jnp.bfloat16
    )
    return (token_grad, gate_grad_out, new_momentum_in, new_momentum_out)


def solution(mesh):
    in_specs = (
        P(("rep", "expert"), None),
        P(("rep", "expert"), None),
        P(("rep", "expert"), None),
        P(("rep", "expert"), None),
        P("expert", "rep", None),
        P("expert", None, "rep"),
        P("expert", "rep", None),
        P("expert", None, "rep"),
    )
    out_specs = (
        P(("rep", "expert"), None),
        P(("rep", "expert"), None),
        P("expert", "rep", None),
        P("expert", None, "rep"),
    )

    small = mesh.shape["expert"] == 8 and mesh.shape["rep"] == 4

    def per_device(*args):
        tok, width = args[0].shape
        w_in, w_out = args[4], args[5]
        lanes = (tok, w_in.shape[1], w_out.shape[1], w_out.shape[2], w_in.shape[2])
        fits = small and tok == 128 and width >= tok and all(n % 128 == 0 for n in lanes)
        dense = fits and w_in.shape[0] == 1 and w_in.shape[1] == w_out.shape[2] == w_out.shape[1]
        return (per_device_dense if dense else per_device_sparse)(*args)

    return jax.shard_map(
        per_device, mesh=mesh, in_specs=in_specs, out_specs=out_specs, check_vma=False
    )
```

```python
import jax
import jax.numpy as jnp
from jax import lax
from jax.experimental import pallas as pl
from jax.experimental.pallas import tpu as pltpu
from jax.sharding import PartitionSpec as P


momentum_decay = 0.9
bf16 = jnp.bfloat16
f32 = jnp.float32
MIB = 1024 * 1024


def dot(a, b, left, right):
    return lax.dot_general(a, b, (((left,), (right,)), ((), ())), preferred_element_type=f32)


def call(kernel, operands, outs, scratch=(), mib=8, scalars=0, flops=0, far=0):
    specs = [pl.BlockSpec(memory_space=pltpu.SMEM)] * scalars
    specs += [pl.BlockSpec(memory_space=pltpu.VMEM)] * (len(operands) - scalars - far)
    specs += [pl.BlockSpec(memory_space=pltpu.HBM)] * far
    return pl.pallas_call(
        kernel,
        out_shape=[jax.ShapeDtypeStruct(shape, dtype) for shape, dtype in outs],
        in_specs=specs,
        out_specs=[pl.BlockSpec(memory_space=pltpu.VMEM)] * len(outs),
        scratch_shapes=[pltpu.VMEM(*item) if isinstance(item, tuple) else item for item in scratch],
        compiler_params=pltpu.CompilerParams(vmem_limit_bytes=mib * MIB),
        cost_estimate=pl.CostEstimate(flops=flops, bytes_accessed=4 * MIB, transcendentals=0),
    )(*operands)


def stage_kernel(routes_hbm, gates_hbm, x_hbm, y_hbm, win_hbm, wout_hbm, *refs):
    x_ref, block_ref, win_ref, wout_ref, routes_ref, gates_ref, y_ref, sems = refs
    tok, width = y_ref.shape
    moves = (
        (routes_hbm, routes_ref),
        (gates_hbm, gates_ref),
        (y_hbm, y_ref),
        (x_hbm, x_ref),
        (win_hbm, win_ref),
        (wout_hbm, wout_ref),
    )
    copies = [pltpu.make_async_copy(src, dst, sems.at[i]) for i, (src, dst) in enumerate(moves)]
    for copy in copies:
        copy.start()
    copies[0].wait()
    copies[1].wait()
    first = width // 128 * tok
    experts = block_ref.shape[0] - first
    ids = lax.broadcasted_iota(jnp.int32, (experts, tok), 0)
    dense = jnp.zeros((experts, tok), f32)
    for k in range(routes_ref.shape[0]):
        gate = gates_ref[k : k + 1, :].astype(f32)
        dense = dense + jnp.where(ids == routes_ref[k : k + 1, :], gate, 0.0)
    block_ref[first:, :] = dense.astype(bf16)
    copies[2].wait()
    for j in range(width // 128):
        block_ref[j * tok : (j + 1) * tok, :] = y_ref[:, j * 128 : (j + 1) * 128]
    for copy in copies[3:]:
        copy.wait()


def stacked(width, tok, experts):
    return (width // 128 * tok + experts, 128)


def unstack(ref, width):
    tok = 128
    return jnp.concatenate([ref[j * tok : (j + 1) * tok, :] for j in range(width // 128)], axis=1)


def gate_column(table, expert):
    pick = lax.broadcasted_iota(jnp.int32, table.shape, 0) == expert
    return jnp.sum(jnp.where(pick, table.astype(f32), 0.0).T, axis=1, keepdims=True)


def gate_table(column, experts, expert):
    spread = jnp.broadcast_to(column, (column.shape[0], experts)).T
    pick = lax.broadcasted_iota(jnp.int32, spread.shape, 0) == expert
    return jnp.where(pick, spread, 0.0)


def write_rows(out, row_grad, table):
    tok, width = row_grad.shape
    for j in range(width // 128):
        out[j * tok : (j + 1) * tok, :] = row_grad[:, j * 128 : (j + 1) * 128]
    out[width // 128 * tok :, :] = table.astype(bf16)


def activations(both):
    ffn = both.shape[1] // 2
    g, u = both[:, :ffn], both[:, ffn:]
    s = 1.0 / (1.0 + jnp.exp(-g))
    silu = g * s
    hidden = (silu * u).astype(bf16)
    return silu, u * s * (1.0 + g * (1.0 - s)), hidden


def back_step(tables, expert, y, acts, win, wout, keep_ref, give_ref, dgu_ref, ch_ref):
    silu, slope, hidden = acts
    tok, ffn, experts = y.shape[0] // 2, wout.shape[0], tables[0].shape[0]
    gate = jnp.concatenate([gate_column(table, expert) for table in tables], axis=0)
    back = dot(y, wout[...], 1, 1)
    gate_grad = jnp.sum(hidden.astype(f32) * back, axis=1, keepdims=True)
    ch_ref[...] = (hidden.astype(f32) * gate).astype(bf16)
    dh = back * gate
    dgu_ref[:, :ffn] = (dh * slope).astype(bf16)
    dgu_ref[:, ffn:] = (dh * silu).astype(bf16)
    row_grad = dot(dgu_ref[...], win[...], 1, 1).astype(bf16)
    for i, out in enumerate((keep_ref, give_ref)):
        part = slice(i * tok, (i + 1) * tok)
        write_rows(out, row_grad[part], gate_table(gate_grad[part], experts, expert))


def own_kernel(ids_ref, x0, x1, y0, y1, *refs):
    in_pieces, out_pieces, refs = refs[0:5], refs[5:9], refs[9:]
    keep_ref, give_ref, dgu_ref, ch_ref, win, wout = refs
    rep, expert = ids_ref[0], ids_ref[1]
    shard, (tok, width) = wout.shape[1] // 4, x0.shape
    cut = in_pieces[3].shape[1]
    for j in range(4):
        at = pl.multiple_of((rep ^ j) * shard, 128)
        wout[:, pl.ds(at, shard)] = out_pieces[j][0]
        if j < 3:
            win[pl.ds(at, shard), :] = in_pieces[j][0]
        else:
            win[pl.ds(at, cut), :] = in_pieces[3][0]
            win[pl.ds(at + cut, shard - cut), :] = in_pieces[4][0]
    tables = [ref[width // 128 * tok :, :] for ref in (y0, y1)]
    x = jnp.concatenate([x0[...], x1[...]], axis=0)
    y = jnp.concatenate([unstack(y0, width), unstack(y1, width)], axis=0)
    acts = activations(dot(x, win[...], 1, 0))
    back_step(tables, expert, y, acts, win, wout, keep_ref, give_ref, dgu_ref, ch_ref)


def early_kernel(n0, n1, f0, f1, win, xs, silu_ref, slope_ref, hidden_ref):
    tok = n0.shape[0]
    for n, ref in enumerate((n0, n1, f0, f1)):
        xs[n * tok : (n + 1) * tok, :] = ref[...]
    silu_ref[...], slope_ref[...], hidden_ref[...] = activations(dot(xs[...], win[...], 1, 0))


def rest_kernel(ids_ref, *refs):
    blocks, (silu, slope, hidden, win, wout), refs = refs[0:4], refs[4:9], refs[9:]
    keep_ref, give_ref, ys, dgus, chs = refs
    rows, width = ys.shape[0] // 2, ys.shape[1]
    tok = rows // 2
    for n in range(2):
        part, pair = slice(n * rows, (n + 1) * rows), blocks[2 * n : 2 * n + 2]
        for i, ref in enumerate(pair):
            ys[n * rows + i * tok : n * rows + (i + 1) * tok, :] = unstack(ref, width)
        tables = [ref[width // 128 * tok :, :] for ref in pair]
        acts = (silu[part, :], slope[part, :], hidden[part, :])
        outs = (keep_ref.at[n], give_ref.at[n], dgus.at[part], chs.at[part])
        back_step(tables, ids_ref[1], ys[part, :], acts, win, wout, *outs)


def sum_kernel(x0, x1, y0, y1, own_dgu, own_ch, more_xs, more_ys, more_dgu, more_ch, *refs):
    acc_in_ref, acc_out_ref, xs, ys, dgus, chs = refs
    tok, width = x0.shape
    rows = 2 * tok
    for i, (x, y) in enumerate(((x0, y0), (x1, y1))):
        xs[i * tok : (i + 1) * tok, :] = x[...]
        ys[i * tok : (i + 1) * tok, :] = unstack(y, width)
    for whole, first, more in ((dgus, own_dgu, more_dgu), (chs, own_ch, more_ch)):
        whole[0:rows, :] = first[...]
        whole[rows:, :] = more[...]
    xs[rows:, :] = more_xs[...]
    ys[rows:, :] = more_ys[...]
    acc_in_ref[...] = dot(xs[...], dgus[...], 0, 0)
    acc_out_ref[...] = dot(chs[...], ys[...], 0, 0)


def forward_kernel(x0, x1, win, xs, silu_ref, slope_ref, hidden_ref):
    tok = x0.shape[0]
    xs[0:tok, :] = x0[...]
    xs[tok:, :] = x1[...]
    silu_ref[...], slope_ref[...], hidden_ref[...] = activations(dot(xs[...], win[...], 1, 0))


def shard_grads(refs, acc_in_ref, acc_out_ref, xs, ys, dgus, chs, index):
    shard = sum(ref.shape[0] for ref in refs)
    at = pl.multiple_of(index * shard, 128)
    part_in = acc_in_ref[pl.ds(at, shard), :] + dot(xs[:, pl.ds(at, shard)], dgus[...], 0, 0)
    part_out = acc_out_ref[:, pl.ds(at, shard)] + dot(chs[...], ys[:, pl.ds(at, shard)], 0, 0)
    cols = part_in.shape[1]
    at = 0
    for ref in refs:
        rows = slice(at, at + ref.shape[0])
        ref[:, 0:cols] = part_in[rows].astype(bf16)
        ref[:, cols:] = part_out[rows].astype(bf16)
        at = rows.stop


def grad_kernel(ids_ref, y0, y1, xs, silu, slope, hidden, wout, acc_in, acc_out, *refs):
    r3a_ref, r3b_ref, dgus, chs, ys, gate_ref = refs
    rep, expert = ids_ref[0], ids_ref[1]
    tok, width = ys.shape[0] // 2, ys.shape[1]
    ffn = wout.shape[0]
    ys[0:tok, :] = unstack(y0, width)
    ys[tok:, :] = unstack(y1, width)
    first = width // 128 * tok
    gate = jnp.concatenate([gate_column(ref[first:, :], expert) for ref in (y0, y1)], axis=0)
    back = dot(ys[...], wout[...], 1, 1)
    gate_grad = jnp.sum(hidden[...].astype(f32) * back, axis=1, keepdims=True)
    chs[...] = (hidden[...].astype(f32) * gate).astype(bf16)
    dh = back * gate
    dgus[:, :ffn] = (dh * slope[...]).astype(bf16)
    dgus[:, ffn:] = (dh * silu[...]).astype(bf16)
    gate_ref[...] = gate_grad
    shard_grads((r3a_ref, r3b_ref), acc_in, acc_out, xs, ys, dgus, chs, rep ^ 3)


def other_grads_kernel(ids_ref, xs, ys, dgus, chs, acc_in, acc_out, mine_ref, r1a_ref, r1b_ref, r2a_ref, r2b_ref):
    rep = ids_ref[0]
    args = (acc_in, acc_out, xs, ys, dgus, chs)
    shard_grads((r1a_ref, r1b_ref), *args, rep ^ 1)
    shard_grads((r2a_ref, r2b_ref), *args, rep ^ 2)
    shard_grads((mine_ref,), *args, rep)


def rows_kernel(ids_ref, dgus, win, gate_ref, keep_ref, give_ref):
    tok, width = dgus.shape[0] // 2, win.shape[0]
    experts = keep_ref.shape[0] - width // 128 * tok
    row_grad = dot(dgus[...], win[...], 1, 1).astype(bf16)
    for i, out in enumerate((keep_ref, give_ref)):
        part = slice(i * tok, (i + 1) * tok)
        write_rows(out, row_grad[part], gate_table(gate_ref[part, :], experts, ids_ref[1]))


def combine_kernel(routes_ref, p0, p1, p2, p3, token_ref, gate_ref):
    tok, width = token_ref.shape
    parts = (p0, p1, p2, p3)
    for j in range(width // 128):
        rows = slice(j * tok, (j + 1) * tok)
        total = sum(p[rows, :].astype(f32) for p in parts)
        token_ref[:, j * 128 : (j + 1) * 128] = total.astype(bf16)
    table = sum(p[width // 128 * tok :, :].astype(f32) for p in parts)
    ids = lax.broadcasted_iota(jnp.int32, table.shape, 0)
    for k in range(routes_ref.shape[0]):
        mine = jnp.where(ids == routes_ref[k : k + 1, :], table, 0.0)
        gate_ref[k : k + 1, :] = jnp.sum(mine, axis=0, keepdims=True).astype(bf16)


def mix_kernel(own_ref, t1b_ref, t2a_ref, min_ref, mout_ref, base_ref):
    cut, cols = t2a_ref.shape[0], min_ref.shape[2]
    for rows, part in ((slice(0, cut), t2a_ref), (slice(cut, own_ref.shape[0]), t1b_ref)):
        total = own_ref[rows, :].astype(f32) + part[...].astype(f32)
        base_ref[rows, 0:cols] = total[:, :cols] + momentum_decay * min_ref[0, rows, :].astype(f32)
        base_ref[rows, cols:] = total[:, cols:] + momentum_decay * mout_ref[0, rows, :].astype(f32)


def finish_kernel(base_ref, t1a_ref, t2b_ref, nin_ref, nout_ref):
    cut, cols = t1a_ref.shape[0], nin_ref.shape[2]
    for rows, part in ((slice(0, cut), t1a_ref), (slice(cut, base_ref.shape[0]), t2b_ref)):
        total = (base_ref[rows, :] + part[...].astype(f32)).astype(bf16)
        nin_ref[0, rows, :] = total[:, :cols]
        nout_ref[0, rows, :] = total[:, cols:]


def per_device_dense(*args):
    return dense_step(*args)


def dense_step(tokens, routes, gates, output_grad, w_in, w_out, momentum_in, momentum_out):
    tok, width = tokens.shape
    ffn, both_w = w_out.shape[1], w_in.shape[2]
    shard = w_in.shape[1]
    cols = both_w + shard
    experts = lax.axis_size("expert")
    chips = experts // 2
    rep = lax.axis_index("rep")
    expert = lax.axis_index("expert")
    ids = jnp.stack([rep, expert]).astype(jnp.int32)

    def over_rep(value, bits):
        return lax.ppermute(value, "rep", [(i, i ^ bits) for i in range(4)])

    def over_chips(value, chip_pairs):
        pairs = [(2 * a + c, 2 * b + c) for a, b in chip_pairs for c in range(2)]
        return lax.ppermute(value, "expert", pairs)

    def partner(value):
        return lax.ppermute(value, "expert", [(i, i ^ 1) for i in range(experts)])

    to_far = [(z, z ^ 2) for z in range(chips)]
    to_near = [(z, z ^ 1) for z in range(chips)]
    to_cross = [(z, z ^ 3) for z in range(chips)]
    to_middle = [(1, 2), (2, 1)]
    to_ends = [(2, 3), (1, 0)]

    far_x = over_chips(tokens, to_far)
    w1in = over_rep(w_in, 1)
    w2in = over_rep(w_in, 2)
    near_x = over_chips(tokens, to_near)
    top = routes.shape[1]
    sources = [routes.T, gates.T, tokens, output_grad, w_in, w_out]
    own_x, own_y, own_in, own_out = call(
        stage_kernel,
        sources,
        [((tok, width), bf16), (stacked(width, tok, experts), bf16)]
        + [(w_in.shape, bf16), (w_out.shape, bf16)],
        [((top, tok), jnp.int32), ((top, tok), bf16), ((tok, width), bf16)]
        + [pltpu.SemaphoreType.DMA((len(sources),))],
        mib=4,
        far=len(sources),
    )
    far_y = over_chips(own_y, to_far)
    near_y = over_chips(own_y, to_near)
    w1out = over_rep(w_out, 1)
    w2out = over_rep(w_out, 2)
    middle_x = over_chips(tokens, to_middle)
    own_xp = partner(own_x)
    own_yp = partner(own_y)
    cut = shard * 3 // 4
    w3ina = over_rep(w1in[:, :cut], 2)
    ends_x = over_chips(far_x, to_ends)
    w3inb = over_rep(w2in[:, cut:], 1)
    w3out = over_rep(w2out, 1)
    far_xp = partner(far_x)
    near_xp = partner(near_x)
    middle_y = over_chips(own_y, to_middle)
    rows = 2 * tok
    block = (stacked(width, tok, experts), bf16)
    flops = 5 * rows * width * both_w
    own_blocks = [own_x, own_xp, own_y, own_yp]
    keep, give_own, own_dgu, own_ch, win, wout = call(
        own_kernel,
        [ids, *own_blocks, own_in, w1in, w2in, w3ina, w3inb, own_out, w1out, w2out, w3out],
        [block, block, ((rows, both_w), bf16), ((rows, ffn), bf16)]
        + [((width, both_w), bf16), ((ffn, width), bf16)],
        mib=10,
        scalars=1,
        flops=flops,
    )
    ends_y = over_chips(far_y, to_ends)
    far_yp = partner(far_y)
    near_yp = partner(near_y)
    got = partner(give_own)
    home_own = (keep.astype(f32) + got.astype(f32)).astype(bf16)
    more_xs, *early = call(
        early_kernel,
        [near_x, near_xp, far_x, far_xp, win],
        [((2 * rows, width), bf16), ((2 * rows, ffn), f32), ((2 * rows, ffn), f32), ((2 * rows, ffn), bf16)],
        mib=6,
        flops=2 * flops // 5 * 2,
    )
    keep, give, *more = call(
        rest_kernel,
        [ids, near_y, near_yp, far_y, far_yp, *early, win, wout],
        [((2, *stacked(width, tok, experts)), bf16)] * 2
        + [((2 * rows, width), bf16), ((2 * rows, both_w), bf16), ((2 * rows, ffn), bf16)],
        mib=8,
        scalars=1,
        flops=flops,
    )
    acc_in, acc_out = call(
        sum_kernel,
        [*own_blocks, own_dgu, own_ch, more_xs, *more],
        [((width, both_w), f32), ((ffn, width), f32)],
        [((3 * rows, n), bf16) for n in (width, width, both_w, ffn)],
        mib=16,
        flops=2 * flops,
    )
    got = partner(give)
    home_near, home_far = ((keep[i].astype(f32) + got[i].astype(f32)).astype(bf16) for i in range(2))
    cross_x = ends_x + middle_x
    cross_xp = partner(cross_x)
    xs, silu, slope, hidden = call(
        forward_kernel,
        [cross_x, cross_xp, win],
        [((rows, width), bf16), ((rows, ffn), f32), ((rows, ffn), f32), ((rows, ffn), bf16)],
        flops=2 * rows * width * both_w,
    )
    cross_y = ends_y + middle_y
    cross_yp = partner(cross_y)
    home_far = over_chips(home_far, to_far)
    home_near = over_chips(home_near, to_near)
    part_a = shard * 13 // 24 // 16 * 16
    part_b = shard - part_a
    r3a, r3b, dgus, chs, ys, gate_last = call(
        grad_kernel,
        [ids, cross_y, cross_yp, xs, silu, slope, hidden, wout]
        + [acc_in, acc_out],
        [((part_a, cols), bf16), ((part_b, cols), bf16)]
        + [((rows, both_w), bf16), ((rows, ffn), bf16), ((rows, width), bf16), ((rows, 1), f32)],
        mib=8,
        scalars=1,
        flops=rows * width * both_w * 2,
    )
    s3a = over_rep(r3a, 2)
    s3b = over_rep(r3b, 1)
    mine, r1a, r1b, r2a, r2b = call(
        other_grads_kernel,
        [ids, xs, ys, dgus, chs, acc_in, acc_out],
        [((shard, cols), bf16)] + [((part_a, cols), bf16), ((part_b, cols), bf16)] * 2,
        mib=8,
        scalars=1,
        flops=2 * rows * width * both_w,
    )
    keep2, give2 = call(rows_kernel, [ids, dgus, win, gate_last], [block, block], scalars=1)
    got2 = partner(give2)
    t2a = over_rep(r2a, 2)
    t1b = over_rep(r1b, 1)
    last = (keep2.astype(f32) + got2.astype(f32)).astype(bf16)
    home_cross = over_chips(last, to_cross)
    t1a = over_rep((r1a.astype(f32) + s3a.astype(f32)).astype(bf16), 1)
    t2b = over_rep((r2b.astype(f32) + s3b.astype(f32)).astype(bf16), 2)
    token_grad, gate_grad = call(
        combine_kernel,
        [routes.T, home_own, home_near, home_far, home_cross],
        [((tok, width), bf16), ((top, tok), bf16)],
        mib=4,
    )
    (base,) = call(mix_kernel, [mine, t1b, t2a, momentum_in, momentum_out], [((shard, cols), f32)])
    new_in, new_out = call(
        finish_kernel, [base, t1a, t2b], [(momentum_in.shape, bf16), (momentum_out.shape, bf16)]
    )
    return token_grad, gate_grad.T, new_in, new_out


def slot_positions(routes, experts):
    flat_routes = routes.reshape(-1)
    one_hot = (flat_routes[:, None] == jnp.arange(experts, dtype=jnp.int32)[None, :]).astype(
        jnp.int32
    )
    earlier = jnp.cumsum(one_hot, axis=0) - one_hot
    return jnp.sum(earlier * one_hot, axis=1)


def forward_pass(x_rows, weight_in, weight_out):
    width_ffn = weight_out.shape[0]
    both = jnp.dot(x_rows, weight_in, preferred_element_type=jnp.float32)
    gate_pre = both[:, :width_ffn]
    up_part = both[:, width_ffn:]
    silu_gate = jax.nn.silu(gate_pre)
    hidden = (silu_gate * up_part).astype(jnp.bfloat16)
    expert_out = jnp.dot(hidden, weight_out, preferred_element_type=jnp.float32)
    return (gate_pre, up_part, silu_gate, hidden, expert_out)


def per_device_sparse(tokens, routes, gates, output_grad, w_in, w_out, momentum_in, momentum_out):
    tok_dev, width = tokens.shape
    top_count = routes.shape[1]
    senders = lax.axis_size("expert")
    local_count = w_in.shape[0]
    experts = senders * local_count
    capacity = max(2, min(tok_dev, 5 * tok_dev * top_count // (4 * experts)))
    slot_count = experts * capacity
    target = routes.reshape(-1) * capacity + slot_positions(routes, experts)
    token_ids = jnp.repeat(jnp.arange(tok_dev, dtype=jnp.int32), top_count)
    source_row = jnp.full((slot_count,), tok_dev, jnp.int32).at[target].set(token_ids)
    slot_gate = jnp.zeros((slot_count,), jnp.bfloat16).at[target].set(gates.reshape(-1))
    zero_row = jnp.zeros((1, width), jnp.bfloat16)
    sent_tokens = jnp.concatenate([tokens, zero_row], axis=0)[source_row].reshape(
        experts, capacity, width
    )
    sent_grads = jnp.concatenate([output_grad, zero_row], axis=0)[source_row].reshape(
        experts, capacity, width
    )
    sent_gate = slot_gate.reshape(experts, capacity)
    whole_in, whole_out = (
        lax.all_gather(w_in, "rep", axis=1, tiled=True),
        lax.all_gather(w_out, "rep", axis=2, tiled=True),
    )

    def local_rows(received, expert):
        shaped = received.reshape((senders, local_count) + received.shape[1:])
        return shaped[:, expert].reshape((senders * capacity,) + received.shape[2:])

    got_tokens, got_grads, got_gate = (
        lax.all_to_all(sent_tokens, "expert", split_axis=0, concat_axis=0, tiled=True),
        lax.all_to_all(sent_grads, "expert", split_axis=0, concat_axis=0, tiled=True),
        lax.all_to_all(sent_gate, "expert", split_axis=0, concat_axis=0, tiled=True),
    )
    forward = [forward_pass(local_rows(got_tokens, 0), whole_in[0], whole_out[0])]
    expert = 0
    gate_pre, up_part, silu_gate, hidden, expert_out = forward[expert]
    dy_rows = local_rows(got_grads, expert)
    gate_grad = jnp.sum(expert_out * dy_rows.astype(jnp.float32), axis=1).astype(jnp.bfloat16)
    scaled = (
        local_rows(got_gate, expert).astype(jnp.float32)[:, None] * dy_rows.astype(jnp.float32)
    ).astype(jnp.bfloat16)
    scaled_rows = [scaled]
    gate_rows = [gate_grad]
    parts_out = [
        lax.dot_general(
            hidden, scaled, (((0,), (0,)), ((), ())), preferred_element_type=jnp.float32
        )
    ]
    grad_out_all = jnp.stack(parts_out)
    summed_out = lax.psum_scatter(
        grad_out_all.astype(jnp.bfloat16), "rep", scatter_dimension=2, tiled=True
    ).astype(jnp.float32)
    expert = 0
    gate_pre, up_part, silu_gate, hidden, expert_out = forward[expert]
    hidden_grad = lax.dot_general(
        scaled_rows[expert],
        whole_out[expert],
        (((1,), (1,)), ((), ())),
        preferred_element_type=jnp.float32,
    )
    sigma = jax.nn.sigmoid(gate_pre)
    dgu = jnp.concatenate(
        [hidden_grad * up_part * sigma * (1.0 + gate_pre * (1.0 - sigma)), hidden_grad * silu_gate],
        axis=1,
    ).astype(jnp.bfloat16)
    row_grad = lax.dot_general(
        dgu, whole_in[expert], (((1,), (1,)), ((), ())), preferred_element_type=jnp.float32
    ).astype(jnp.bfloat16)
    row_grads = row_grad.reshape(senders, 1, capacity, width)
    parts_in = [
        lax.dot_general(
            local_rows(got_tokens, expert),
            dgu,
            (((0,), (0,)), ((), ())),
            preferred_element_type=jnp.float32,
        )
    ]
    grad_in_all = jnp.stack(parts_in)
    back_send = row_grads.reshape(experts, capacity, width)
    gate_send = jnp.stack([item.reshape(senders, capacity) for item in gate_rows], axis=1).reshape(
        experts, capacity
    )
    back_rows, back_gate = (
        lax.all_to_all(back_send, "expert", split_axis=0, concat_axis=0, tiled=True),
        lax.all_to_all(gate_send, "expert", split_axis=0, concat_axis=0, tiled=True),
    )
    picked = back_rows.reshape(slot_count, width)[target].reshape(tok_dev, top_count, width)
    token_grad = jnp.sum(picked.astype(jnp.float32), axis=1).astype(jnp.bfloat16)
    gate_grad_out = back_gate.reshape(-1)[target].reshape(tok_dev, top_count)
    summed_in = lax.psum_scatter(
        grad_in_all.astype(jnp.bfloat16), "rep", scatter_dimension=1, tiled=True
    ).astype(jnp.float32)
    new_momentum_in = (momentum_decay * momentum_in.astype(jnp.float32) + summed_in).astype(
        jnp.bfloat16
    )
    new_momentum_out = (momentum_decay * momentum_out.astype(jnp.float32) + summed_out).astype(
        jnp.bfloat16
    )
    return (token_grad, gate_grad_out, new_momentum_in, new_momentum_out)


def solution(mesh):
    in_specs = (
        P(("rep", "expert"), None),
        P(("rep", "expert"), None),
        P(("rep", "expert"), None),
        P(("rep", "expert"), None),
        P("expert", "rep", None),
        P("expert", None, "rep"),
        P("expert", "rep", None),
        P("expert", None, "rep"),
    )
    out_specs = (
        P(("rep", "expert"), None),
        P(("rep", "expert"), None),
        P("expert", "rep", None),
        P("expert", None, "rep"),
    )

    small = mesh.shape["expert"] == 8 and mesh.shape["rep"] == 4

    def per_device(*args):
        tok, width = args[0].shape
        w_in, w_out = args[4], args[5]
        lanes = (tok, w_in.shape[1], w_out.shape[1], w_out.shape[2], w_in.shape[2])
        fits = small and tok == 128 and width >= tok and all(n % 128 == 0 for n in lanes)
        dense = fits and w_in.shape[0] == 1 and w_in.shape[1] == w_out.shape[2] == w_out.shape[1]
        return (per_device_dense if dense else per_device_sparse)(*args)

    return jax.shard_map(
        per_device, mesh=mesh, in_specs=in_specs, out_specs=out_specs, check_vma=False
    )
```

```python
import jax
import jax.numpy as jnp
from jax import lax
from jax.experimental import pallas as pl
from jax.experimental.pallas import tpu as pltpu
from jax.sharding import PartitionSpec as P


momentum_decay = 0.9
bf16 = jnp.bfloat16
f32 = jnp.float32
MIB = 1024 * 1024


def dot(a, b, left, right):
    return lax.dot_general(a, b, (((left,), (right,)), ((), ())), preferred_element_type=f32)


def call(kernel, operands, outs, scratch=(), mib=8, scalars=0, flops=0, far=0):
    specs = [pl.BlockSpec(memory_space=pltpu.SMEM)] * scalars
    specs += [pl.BlockSpec(memory_space=pltpu.VMEM)] * (len(operands) - scalars - far)
    specs += [pl.BlockSpec(memory_space=pltpu.HBM)] * far
    return pl.pallas_call(
        kernel,
        out_shape=[jax.ShapeDtypeStruct(shape, dtype) for shape, dtype in outs],
        in_specs=specs,
        out_specs=[pl.BlockSpec(memory_space=pltpu.VMEM)] * len(outs),
        scratch_shapes=[pltpu.VMEM(*item) if isinstance(item, tuple) else item for item in scratch],
        compiler_params=pltpu.CompilerParams(vmem_limit_bytes=mib * MIB),
        cost_estimate=pl.CostEstimate(flops=flops, bytes_accessed=4 * MIB, transcendentals=0),
    )(*operands)


def stage_kernel(routes_hbm, gates_hbm, x_hbm, y_hbm, win_hbm, wout_hbm, *refs):
    x_ref, block_ref, win_ref, wout_ref, routes_ref, gates_ref, y_ref, sems = refs
    tok, width = y_ref.shape
    moves = (
        (routes_hbm, routes_ref),
        (gates_hbm, gates_ref),
        (y_hbm, y_ref),
        (x_hbm, x_ref),
        (win_hbm, win_ref),
        (wout_hbm, wout_ref),
    )
    copies = [pltpu.make_async_copy(src, dst, sems.at[i]) for i, (src, dst) in enumerate(moves)]
    for copy in copies:
        copy.start()
    copies[0].wait()
    copies[1].wait()
    first = width // 128 * tok
    experts = block_ref.shape[0] - first
    ids = lax.broadcasted_iota(jnp.int32, (experts, tok), 0)
    dense = jnp.zeros((experts, tok), f32)
    for k in range(routes_ref.shape[0]):
        gate = gates_ref[k : k + 1, :].astype(f32)
        dense = dense + jnp.where(ids == routes_ref[k : k + 1, :], gate, 0.0)
    block_ref[first:, :] = dense.astype(bf16)
    copies[2].wait()
    for j in range(width // 128):
        block_ref[j * tok : (j + 1) * tok, :] = y_ref[:, j * 128 : (j + 1) * 128]
    for copy in copies[3:]:
        copy.wait()


def stacked(width, tok, experts):
    return (width // 128 * tok + experts, 128)


def unstack(ref, width):
    tok = 128
    return jnp.concatenate([ref[j * tok : (j + 1) * tok, :] for j in range(width // 128)], axis=1)


def gate_column(table, expert):
    pick = lax.broadcasted_iota(jnp.int32, table.shape, 0) == expert
    return jnp.sum(jnp.where(pick, table.astype(f32), 0.0).T, axis=1, keepdims=True)


def gate_table(column, experts, expert):
    spread = jnp.broadcast_to(column, (column.shape[0], experts)).T
    pick = lax.broadcasted_iota(jnp.int32, spread.shape, 0) == expert
    return jnp.where(pick, spread, 0.0)


def write_rows(out, row_grad, table):
    tok, width = row_grad.shape
    for j in range(width // 128):
        out[j * tok : (j + 1) * tok, :] = row_grad[:, j * 128 : (j + 1) * 128]
    out[width // 128 * tok :, :] = table.astype(bf16)


def activations(both):
    ffn = both.shape[1] // 2
    g, u = both[:, :ffn], both[:, ffn:]
    s = 1.0 / (1.0 + jnp.exp(-g))
    silu = g * s
    hidden = (silu * u).astype(bf16)
    return silu, u * s * (1.0 + g * (1.0 - s)), hidden


def back_step(tables, expert, y, acts, win, wout, keep_ref, give_ref, dgu_ref, ch_ref):
    silu, slope, hidden = acts
    tok, ffn, experts = y.shape[0] // 2, wout.shape[0], tables[0].shape[0]
    gate = jnp.concatenate([gate_column(table, expert) for table in tables], axis=0)
    back = dot(y, wout[...], 1, 1)
    gate_grad = jnp.sum(hidden.astype(f32) * back, axis=1, keepdims=True)
    ch_ref[...] = (hidden.astype(f32) * gate).astype(bf16)
    dh = back * gate
    dgu_ref[:, :ffn] = (dh * slope).astype(bf16)
    dgu_ref[:, ffn:] = (dh * silu).astype(bf16)
    row_grad = dot(dgu_ref[...], win[...], 1, 1).astype(bf16)
    for i, out in enumerate((keep_ref, give_ref)):
        part = slice(i * tok, (i + 1) * tok)
        write_rows(out, row_grad[part], gate_table(gate_grad[part], experts, expert))


def own_kernel(ids_ref, x0, x1, y0, y1, *refs):
    in_pieces, out_pieces, refs = refs[0:5], refs[5:9], refs[9:]
    keep_ref, give_ref, dgu_ref, ch_ref, win, wout = refs
    rep, expert = ids_ref[0], ids_ref[1]
    shard, (tok, width) = wout.shape[1] // 4, x0.shape
    cut = in_pieces[3].shape[1]
    for j in range(4):
        at = pl.multiple_of((rep ^ j) * shard, 128)
        wout[:, pl.ds(at, shard)] = out_pieces[j][0]
        if j < 3:
            win[pl.ds(at, shard), :] = in_pieces[j][0]
        else:
            win[pl.ds(at, cut), :] = in_pieces[3][0]
            win[pl.ds(at + cut, shard - cut), :] = in_pieces[4][0]
    tables = [ref[width // 128 * tok :, :] for ref in (y0, y1)]
    x = jnp.concatenate([x0[...], x1[...]], axis=0)
    y = jnp.concatenate([unstack(y0, width), unstack(y1, width)], axis=0)
    acts = activations(dot(x, win[...], 1, 0))
    back_step(tables, expert, y, acts, win, wout, keep_ref, give_ref, dgu_ref, ch_ref)


def early_kernel(n0, n1, f0, f1, win, xs, silu_ref, slope_ref, hidden_ref):
    tok = n0.shape[0]
    for n, ref in enumerate((n0, n1, f0, f1)):
        xs[n * tok : (n + 1) * tok, :] = ref[...]
    silu_ref[...], slope_ref[...], hidden_ref[...] = activations(dot(xs[...], win[...], 1, 0))


def rest_kernel(ids_ref, *refs):
    blocks, (silu, slope, hidden, win, wout), refs = refs[0:4], refs[4:9], refs[9:]
    keep_ref, give_ref, ys, dgus, chs = refs
    rows, width = ys.shape[0] // 2, ys.shape[1]
    tok = rows // 2
    for n in range(2):
        part, pair = slice(n * rows, (n + 1) * rows), blocks[2 * n : 2 * n + 2]
        for i, ref in enumerate(pair):
            ys[n * rows + i * tok : n * rows + (i + 1) * tok, :] = unstack(ref, width)
        tables = [ref[width // 128 * tok :, :] for ref in pair]
        acts = (silu[part, :], slope[part, :], hidden[part, :])
        outs = (keep_ref.at[n], give_ref.at[n], dgus.at[part], chs.at[part])
        back_step(tables, ids_ref[1], ys[part, :], acts, win, wout, *outs)


def sum_kernel(x0, x1, y0, y1, own_dgu, own_ch, more_xs, more_ys, more_dgu, more_ch, *refs):
    acc_in_ref, acc_out_ref, xs, ys, dgus, chs = refs
    tok, width = x0.shape
    rows = 2 * tok
    for i, (x, y) in enumerate(((x0, y0), (x1, y1))):
        xs[i * tok : (i + 1) * tok, :] = x[...]
        ys[i * tok : (i + 1) * tok, :] = unstack(y, width)
    for whole, first, more in ((dgus, own_dgu, more_dgu), (chs, own_ch, more_ch)):
        whole[0:rows, :] = first[...]
        whole[rows:, :] = more[...]
    xs[rows:, :] = more_xs[...]
    ys[rows:, :] = more_ys[...]
    acc_in_ref[...] = dot(xs[...], dgus[...], 0, 0)
    acc_out_ref[...] = dot(chs[...], ys[...], 0, 0)


def forward_kernel(x0, x1, win, xs, silu_ref, slope_ref, hidden_ref):
    tok = x0.shape[0]
    xs[0:tok, :] = x0[...]
    xs[tok:, :] = x1[...]
    silu_ref[...], slope_ref[...], hidden_ref[...] = activations(dot(xs[...], win[...], 1, 0))


def shard_grads(refs, acc_in_ref, acc_out_ref, xs, ys, dgus, chs, index):
    shard = sum(ref.shape[0] for ref in refs)
    at = pl.multiple_of(index * shard, 128)
    part_in = acc_in_ref[pl.ds(at, shard), :] + dot(xs[:, pl.ds(at, shard)], dgus[...], 0, 0)
    part_out = acc_out_ref[:, pl.ds(at, shard)] + dot(chs[...], ys[:, pl.ds(at, shard)], 0, 0)
    cols = part_in.shape[1]
    at = 0
    for ref in refs:
        rows = slice(at, at + ref.shape[0])
        ref[:, 0:cols] = part_in[rows].astype(bf16)
        ref[:, cols:] = part_out[rows].astype(bf16)
        at = rows.stop


def grad_kernel(y0, y1, xs, silu, slope, hidden, wout, acc_in, acc_out, *refs):
    r3a_ref, r3b_ref, dgus, chs, ys, gate_ref = refs
    rep, expert = lax.axis_index("rep"), lax.axis_index("expert")
    tok, width = ys.shape[0] // 2, ys.shape[1]
    ffn = wout.shape[0]
    ys[0:tok, :] = unstack(y0, width)
    ys[tok:, :] = unstack(y1, width)
    first = width // 128 * tok
    gate = jnp.concatenate([gate_column(ref[first:, :], expert) for ref in (y0, y1)], axis=0)
    back = dot(ys[...], wout[...], 1, 1)
    gate_grad = jnp.sum(hidden[...].astype(f32) * back, axis=1, keepdims=True)
    chs[...] = (hidden[...].astype(f32) * gate).astype(bf16)
    dh = back * gate
    dgus[:, :ffn] = (dh * slope[...]).astype(bf16)
    dgus[:, ffn:] = (dh * silu[...]).astype(bf16)
    gate_ref[...] = gate_grad
    shard_grads((r3a_ref, r3b_ref), acc_in, acc_out, xs, ys, dgus, chs, rep ^ 3)


def other_grads_kernel(xs, ys, dgus, chs, acc_in, acc_out, mine_ref, r1a_ref, r1b_ref, r2a_ref, r2b_ref):
    rep = lax.axis_index("rep")
    args = (acc_in, acc_out, xs, ys, dgus, chs)
    shard_grads((r1a_ref, r1b_ref), *args, rep ^ 1)
    shard_grads((r2a_ref, r2b_ref), *args, rep ^ 2)
    shard_grads((mine_ref,), *args, rep)


def rows_kernel(dgus, win, gate_ref, keep_ref, give_ref):
    tok, width = dgus.shape[0] // 2, win.shape[0]
    experts = keep_ref.shape[0] - width // 128 * tok
    row_grad = dot(dgus[...], win[...], 1, 1).astype(bf16)
    for i, out in enumerate((keep_ref, give_ref)):
        part = slice(i * tok, (i + 1) * tok)
        write_rows(out, row_grad[part], gate_table(gate_ref[part, :], experts, lax.axis_index("expert")))


def combine_kernel(routes_ref, p0, p1, p2, p3, token_ref, gate_ref):
    tok, width = token_ref.shape
    parts = (p0, p1, p2, p3)
    for j in range(width // 128):
        rows = slice(j * tok, (j + 1) * tok)
        total = sum(p[rows, :].astype(f32) for p in parts)
        token_ref[:, j * 128 : (j + 1) * 128] = total.astype(bf16)
    table = sum(p[width // 128 * tok :, :].astype(f32) for p in parts)
    ids = lax.broadcasted_iota(jnp.int32, table.shape, 0)
    for k in range(routes_ref.shape[0]):
        mine = jnp.where(ids == routes_ref[k : k + 1, :], table, 0.0)
        gate_ref[k : k + 1, :] = jnp.sum(mine, axis=0, keepdims=True).astype(bf16)


def mix_kernel(own_ref, t1b_ref, t2a_ref, min_ref, mout_ref, base_ref):
    cut, cols = t2a_ref.shape[0], min_ref.shape[2]
    for rows, part in ((slice(0, cut), t2a_ref), (slice(cut, own_ref.shape[0]), t1b_ref)):
        total = own_ref[rows, :].astype(f32) + part[...].astype(f32)
        base_ref[rows, 0:cols] = total[:, :cols] + momentum_decay * min_ref[0, rows, :].astype(f32)
        base_ref[rows, cols:] = total[:, cols:] + momentum_decay * mout_ref[0, rows, :].astype(f32)


def finish_kernel(base_ref, t1a_ref, t2b_ref, nin_ref, nout_ref):
    cut, cols = t1a_ref.shape[0], nin_ref.shape[2]
    for rows, part in ((slice(0, cut), t1a_ref), (slice(cut, base_ref.shape[0]), t2b_ref)):
        total = (base_ref[rows, :] + part[...].astype(f32)).astype(bf16)
        nin_ref[0, rows, :] = total[:, :cols]
        nout_ref[0, rows, :] = total[:, cols:]


def per_device_dense(*args):
    return dense_step(*args)


def dense_step(tokens, routes, gates, output_grad, w_in, w_out, momentum_in, momentum_out):
    tok, width = tokens.shape
    ffn, both_w = w_out.shape[1], w_in.shape[2]
    shard = w_in.shape[1]
    cols = both_w + shard
    experts = lax.axis_size("expert")
    chips = experts // 2
    rep = lax.axis_index("rep")
    expert = lax.axis_index("expert")
    ids = jnp.stack([rep, expert]).astype(jnp.int32)

    def over_rep(value, bits):
        return lax.ppermute(value, "rep", [(i, i ^ bits) for i in range(4)])

    def over_chips(value, chip_pairs):
        pairs = [(2 * a + c, 2 * b + c) for a, b in chip_pairs for c in range(2)]
        return lax.ppermute(value, "expert", pairs)

    def partner(value):
        return lax.ppermute(value, "expert", [(i, i ^ 1) for i in range(experts)])

    to_far = [(z, z ^ 2) for z in range(chips)]
    to_near = [(z, z ^ 1) for z in range(chips)]
    to_cross = [(z, z ^ 3) for z in range(chips)]
    to_middle = [(1, 2), (2, 1)]
    to_ends = [(2, 3), (1, 0)]

    far_x = over_chips(tokens, to_far)
    w1in = over_rep(w_in, 1)
    w2in = over_rep(w_in, 2)
    near_x = over_chips(tokens, to_near)
    top = routes.shape[1]
    sources = [routes.T, gates.T, tokens, output_grad, w_in, w_out]
    own_x, own_y, own_in, own_out = call(
        stage_kernel,
        sources,
        [((tok, width), bf16), (stacked(width, tok, experts), bf16)]
        + [(w_in.shape, bf16), (w_out.shape, bf16)],
        [((top, tok), jnp.int32), ((top, tok), bf16), ((tok, width), bf16)]
        + [pltpu.SemaphoreType.DMA((len(sources),))],
        mib=4,
        far=len(sources),
    )
    far_y = over_chips(own_y, to_far)
    near_y = over_chips(own_y, to_near)
    w1out = over_rep(w_out, 1)
    w2out = over_rep(w_out, 2)
    middle_x = over_chips(tokens, to_middle)
    own_xp = partner(own_x)
    own_yp = partner(own_y)
    cut = shard * 3 // 4
    w3ina = over_rep(w1in[:, :cut], 2)
    ends_x = over_chips(far_x, to_ends)
    w3inb = over_rep(w2in[:, cut:], 1)
    w3out = over_rep(w2out, 1)
    far_xp = partner(far_x)
    near_xp = partner(near_x)
    middle_y = over_chips(own_y, to_middle)
    rows = 2 * tok
    block = (stacked(width, tok, experts), bf16)
    flops = 5 * rows * width * both_w
    own_blocks = [own_x, own_xp, own_y, own_yp]
    keep, give_own, own_dgu, own_ch, win, wout = call(
        own_kernel,
        [ids, *own_blocks, own_in, w1in, w2in, w3ina, w3inb, own_out, w1out, w2out, w3out],
        [block, block, ((rows, both_w), bf16), ((rows, ffn), bf16)]
        + [((width, both_w), bf16), ((ffn, width), bf16)],
        mib=10,
        scalars=1,
        flops=flops,
    )
    ends_y = over_chips(far_y, to_ends)
    far_yp = partner(far_y)
    near_yp = partner(near_y)
    got = partner(give_own)
    home_own = (keep.astype(f32) + got.astype(f32)).astype(bf16)
    more_xs, *early = call(
        early_kernel,
        [near_x, near_xp, far_x, far_xp, win],
        [((2 * rows, width), bf16), ((2 * rows, ffn), f32), ((2 * rows, ffn), f32), ((2 * rows, ffn), bf16)],
        mib=6,
        flops=2 * flops // 5 * 2,
    )
    keep, give, *more = call(
        rest_kernel,
        [ids, near_y, near_yp, far_y, far_yp, *early, win, wout],
        [((2, *stacked(width, tok, experts)), bf16)] * 2
        + [((2 * rows, width), bf16), ((2 * rows, both_w), bf16), ((2 * rows, ffn), bf16)],
        mib=8,
        scalars=1,
        flops=flops,
    )
    acc_in, acc_out = call(
        sum_kernel,
        [*own_blocks, own_dgu, own_ch, more_xs, *more],
        [((width, both_w), f32), ((ffn, width), f32)],
        [((3 * rows, n), bf16) for n in (width, width, both_w, ffn)],
        mib=16,
        flops=2 * flops,
    )
    got = partner(give)
    home_near, home_far = ((keep[i].astype(f32) + got[i].astype(f32)).astype(bf16) for i in range(2))
    cross_x = ends_x + middle_x
    cross_xp = partner(cross_x)
    xs, silu, slope, hidden = call(
        forward_kernel,
        [cross_x, cross_xp, win],
        [((rows, width), bf16), ((rows, ffn), f32), ((rows, ffn), f32), ((rows, ffn), bf16)],
        flops=2 * rows * width * both_w,
    )
    cross_y = ends_y + middle_y
    cross_yp = partner(cross_y)
    home_far = over_chips(home_far, to_far)
    home_near = over_chips(home_near, to_near)
    part_a = shard * 13 // 24 // 16 * 16
    part_b = shard - part_a
    r3a, r3b, dgus, chs, ys, gate_last = call(
        grad_kernel,
        [cross_y, cross_yp, xs, silu, slope, hidden, wout]
        + [acc_in, acc_out],
        [((part_a, cols), bf16), ((part_b, cols), bf16)]
        + [((rows, both_w), bf16), ((rows, ffn), bf16), ((rows, width), bf16), ((rows, 1), f32)],
        mib=8,
        flops=rows * width * both_w * 2,
    )
    s3a = over_rep(r3a, 2)
    s3b = over_rep(r3b, 1)
    mine, r1a, r1b, r2a, r2b = call(
        other_grads_kernel,
        [xs, ys, dgus, chs, acc_in, acc_out],
        [((shard, cols), bf16)] + [((part_a, cols), bf16), ((part_b, cols), bf16)] * 2,
        mib=8,
        flops=2 * rows * width * both_w,
    )
    keep2, give2 = call(rows_kernel, [dgus, win, gate_last], [block, block])
    got2 = partner(give2)
    t2a = over_rep(r2a, 2)
    t1b = over_rep(r1b, 1)
    last = (keep2.astype(f32) + got2.astype(f32)).astype(bf16)
    home_cross = over_chips(last, to_cross)
    t1a = over_rep((r1a.astype(f32) + s3a.astype(f32)).astype(bf16), 1)
    t2b = over_rep((r2b.astype(f32) + s3b.astype(f32)).astype(bf16), 2)
    token_grad, gate_grad = call(
        combine_kernel,
        [routes.T, home_own, home_near, home_far, home_cross],
        [((tok, width), bf16), ((top, tok), bf16)],
        mib=4,
    )
    (base,) = call(mix_kernel, [mine, t1b, t2a, momentum_in, momentum_out], [((shard, cols), f32)])
    new_in, new_out = call(
        finish_kernel, [base, t1a, t2b], [(momentum_in.shape, bf16), (momentum_out.shape, bf16)]
    )
    return token_grad, gate_grad.T, new_in, new_out


def slot_positions(routes, experts):
    flat_routes = routes.reshape(-1)
    one_hot = (flat_routes[:, None] == jnp.arange(experts, dtype=jnp.int32)[None, :]).astype(
        jnp.int32
    )
    earlier = jnp.cumsum(one_hot, axis=0) - one_hot
    return jnp.sum(earlier * one_hot, axis=1)


def forward_pass(x_rows, weight_in, weight_out):
    width_ffn = weight_out.shape[0]
    both = jnp.dot(x_rows, weight_in, preferred_element_type=jnp.float32)
    gate_pre = both[:, :width_ffn]
    up_part = both[:, width_ffn:]
    silu_gate = jax.nn.silu(gate_pre)
    hidden = (silu_gate * up_part).astype(jnp.bfloat16)
    expert_out = jnp.dot(hidden, weight_out, preferred_element_type=jnp.float32)
    return (gate_pre, up_part, silu_gate, hidden, expert_out)


def per_device_sparse(tokens, routes, gates, output_grad, w_in, w_out, momentum_in, momentum_out):
    tok_dev, width = tokens.shape
    top_count = routes.shape[1]
    senders = lax.axis_size("expert")
    local_count = w_in.shape[0]
    experts = senders * local_count
    capacity = max(2, min(tok_dev, 5 * tok_dev * top_count // (4 * experts)))
    slot_count = experts * capacity
    target = routes.reshape(-1) * capacity + slot_positions(routes, experts)
    token_ids = jnp.repeat(jnp.arange(tok_dev, dtype=jnp.int32), top_count)
    source_row = jnp.full((slot_count,), tok_dev, jnp.int32).at[target].set(token_ids)
    slot_gate = jnp.zeros((slot_count,), jnp.bfloat16).at[target].set(gates.reshape(-1))
    zero_row = jnp.zeros((1, width), jnp.bfloat16)
    sent_tokens = jnp.concatenate([tokens, zero_row], axis=0)[source_row].reshape(
        experts, capacity, width
    )
    sent_grads = jnp.concatenate([output_grad, zero_row], axis=0)[source_row].reshape(
        experts, capacity, width
    )
    sent_gate = slot_gate.reshape(experts, capacity)
    whole_in, whole_out = (
        lax.all_gather(w_in, "rep", axis=1, tiled=True),
        lax.all_gather(w_out, "rep", axis=2, tiled=True),
    )

    def local_rows(received, expert):
        shaped = received.reshape((senders, local_count) + received.shape[1:])
        return shaped[:, expert].reshape((senders * capacity,) + received.shape[2:])

    got_tokens, got_grads, got_gate = (
        lax.all_to_all(sent_tokens, "expert", split_axis=0, concat_axis=0, tiled=True),
        lax.all_to_all(sent_grads, "expert", split_axis=0, concat_axis=0, tiled=True),
        lax.all_to_all(sent_gate, "expert", split_axis=0, concat_axis=0, tiled=True),
    )
    forward = [forward_pass(local_rows(got_tokens, 0), whole_in[0], whole_out[0])]
    expert = 0
    gate_pre, up_part, silu_gate, hidden, expert_out = forward[expert]
    dy_rows = local_rows(got_grads, expert)
    gate_grad = jnp.sum(expert_out * dy_rows.astype(jnp.float32), axis=1).astype(jnp.bfloat16)
    scaled = (
        local_rows(got_gate, expert).astype(jnp.float32)[:, None] * dy_rows.astype(jnp.float32)
    ).astype(jnp.bfloat16)
    scaled_rows = [scaled]
    gate_rows = [gate_grad]
    parts_out = [
        lax.dot_general(
            hidden, scaled, (((0,), (0,)), ((), ())), preferred_element_type=jnp.float32
        )
    ]
    grad_out_all = jnp.stack(parts_out)
    summed_out = lax.psum_scatter(
        grad_out_all.astype(jnp.bfloat16), "rep", scatter_dimension=2, tiled=True
    ).astype(jnp.float32)
    expert = 0
    gate_pre, up_part, silu_gate, hidden, expert_out = forward[expert]
    hidden_grad = lax.dot_general(
        scaled_rows[expert],
        whole_out[expert],
        (((1,), (1,)), ((), ())),
        preferred_element_type=jnp.float32,
    )
    sigma = jax.nn.sigmoid(gate_pre)
    dgu = jnp.concatenate(
        [hidden_grad * up_part * sigma * (1.0 + gate_pre * (1.0 - sigma)), hidden_grad * silu_gate],
        axis=1,
    ).astype(jnp.bfloat16)
    row_grad = lax.dot_general(
        dgu, whole_in[expert], (((1,), (1,)), ((), ())), preferred_element_type=jnp.float32
    ).astype(jnp.bfloat16)
    row_grads = row_grad.reshape(senders, 1, capacity, width)
    parts_in = [
        lax.dot_general(
            local_rows(got_tokens, expert),
            dgu,
            (((0,), (0,)), ((), ())),
            preferred_element_type=jnp.float32,
        )
    ]
    grad_in_all = jnp.stack(parts_in)
    back_send = row_grads.reshape(experts, capacity, width)
    gate_send = jnp.stack([item.reshape(senders, capacity) for item in gate_rows], axis=1).reshape(
        experts, capacity
    )
    back_rows, back_gate = (
        lax.all_to_all(back_send, "expert", split_axis=0, concat_axis=0, tiled=True),
        lax.all_to_all(gate_send, "expert", split_axis=0, concat_axis=0, tiled=True),
    )
    picked = back_rows.reshape(slot_count, width)[target].reshape(tok_dev, top_count, width)
    token_grad = jnp.sum(picked.astype(jnp.float32), axis=1).astype(jnp.bfloat16)
    gate_grad_out = back_gate.reshape(-1)[target].reshape(tok_dev, top_count)
    summed_in = lax.psum_scatter(
        grad_in_all.astype(jnp.bfloat16), "rep", scatter_dimension=1, tiled=True
    ).astype(jnp.float32)
    new_momentum_in = (momentum_decay * momentum_in.astype(jnp.float32) + summed_in).astype(
        jnp.bfloat16
    )
    new_momentum_out = (momentum_decay * momentum_out.astype(jnp.float32) + summed_out).astype(
        jnp.bfloat16
    )
    return (token_grad, gate_grad_out, new_momentum_in, new_momentum_out)


def solution(mesh):
    in_specs = (
        P(("rep", "expert"), None),
        P(("rep", "expert"), None),
        P(("rep", "expert"), None),
        P(("rep", "expert"), None),
        P("expert", "rep", None),
        P("expert", None, "rep"),
        P("expert", "rep", None),
        P("expert", None, "rep"),
    )
    out_specs = (
        P(("rep", "expert"), None),
        P(("rep", "expert"), None),
        P("expert", "rep", None),
        P("expert", None, "rep"),
    )

    small = mesh.shape["expert"] == 8 and mesh.shape["rep"] == 4

    def per_device(*args):
        tok, width = args[0].shape
        w_in, w_out = args[4], args[5]
        lanes = (tok, w_in.shape[1], w_out.shape[1], w_out.shape[2], w_in.shape[2])
        fits = small and tok == 128 and width >= tok and all(n % 128 == 0 for n in lanes)
        dense = fits and w_in.shape[0] == 1 and w_in.shape[1] == w_out.shape[2] == w_out.shape[1]
        return (per_device_dense if dense else per_device_sparse)(*args)

    return jax.shard_map(
        per_device, mesh=mesh, in_specs=in_specs, out_specs=out_specs, check_vma=False
    )
```
